256 devices in a mesh: gx: 8 (over x, core), gy: 4 (over z_hi), gz: 8 (over y, z_lo).
Axes of the slice: x: 4, y: 4, z: 8 (z_hi: 4, z_lo: 2; z = z_hi * 2 + z_lo), core: 2. Of those that a mesh axis runs over, the one named last changes fastest.
Arguments:
- occupied: float32 [16, 32, 16, 1024], P(None, 'gx', 'gy', 'gz'), may hold values from -6 to 6
- virtual: float32 [16, 32, 16, 1024], P(None, 'gx', 'gy', 'gz'), may hold values from -6 to 6
- kernel_fields: float32 [4, 32, 16, 1024], P(None, 'gx', 'gy', 'gz'), may hold values from -1.5 to 1.5
- density_grad: float32 [3, 32, 16, 1024], P(None, 'gx', 'gy', 'gz'), may hold values from -6 to 6
Outputs:
- potential: float32 [256, 32, 16, 1024], P(None, 'gx', 'gy', 'gz')
- casida: float32 [256, 256], P(('gx', 'gy', 'gz'))
The draws below stay inside these ranges and needn't reach their ends.
All inputs are finite; a program needn't handle non-finite values.
Results may differ from the reference program's by a relative error of at most 0.00013.
Values sent between devices are 32-bit elements; how exact they have to be, the bound alone decides.
A program may use at most 64 MiB of HBM per device.

```python
import jax
import jax.numpy as jnp
from jax import lax

NOCC = 16
NVIR = 16
NX = 32
NY = 16
NZ = 1024


def steps_of(rng, extent, split, low, high):
    loudness = 1.0
    for axis_at, blocks in split:
        steps = jax.random.uniform(jax.random.fold_in(jax.random.fold_in(rng, 6), axis_at), (blocks,), jnp.float32, low / len(split), high / len(split))
        loudness = loudness * jnp.repeat(jnp.exp(steps), extent[axis_at] // blocks).reshape((-1,) + (1,) * (len(extent) - 1 - axis_at))
    return loudness


def scatter_about(own_key, extent, scale, most, split=(), held_as=jnp.bfloat16):
    gain = steps_of(own_key, extent, split, -0.22, 0.18) if split else 1.0
    array = jax.random.normal(own_key, extent, jnp.float32) * scale * gain
    return jnp.minimum(jnp.maximum(array, -most), most).astype(held_as)


def setup_inputs(seed: int = 0) -> dict:
    keys = jax.random.split(jax.random.key(seed), 5)
    occupied = scatter_about(keys[0], (NOCC, NX, NY, NZ), 1.0, 6.0, ((1, 8), (2, 4), (3, 8)), jnp.float32)
    virtual = scatter_about(keys[1], (NVIR, NX, NY, NZ), 1.0, 6.0, ((1, 8), (2, 4), (3, 8)), jnp.float32)
    kernel_fields = jnp.clip(jax.random.uniform(keys[2], (4, NX, NY, NZ), jnp.float32, -1.5, 1.5) * steps_of(keys[2], (4, NX, NY, NZ), ((1, 8), (2, 4), (3, 8)), -0.4, 0.0), -1.5, 1.5)
    density_grad = scatter_about(keys[3], (3, NX, NY, NZ), 1.0, 6.0, ((1, 8), (2, 4), (3, 8)), jnp.float32)
    return {"occupied": occupied, "virtual": virtual, "kernel_fields": kernel_fields, "density_grad": density_grad}


def derivative(values, dimension):
    inner_diff = jnp.roll(values, -1, dimension) - jnp.roll(values, 1, dimension)
    outer_diff = jnp.roll(values, -2, dimension) - jnp.roll(values, 2, dimension)
    return (8.0 * inner_diff - outer_diff) / 12.0


def respond(densities, kernel_fields, density_grad):
    slopes = [derivative(densities, dimension + 1) for dimension in range(3)]
    aligned = density_grad[0] * slopes[0] + density_grad[1] * slopes[1] + density_grad[2] * slopes[2]
    scalar = kernel_fields[1] * densities + kernel_fields[2] * aligned
    fluxes = [scalar * density_grad[dimension] + kernel_fields[3] * slopes[dimension] for dimension in range(3)]
    divergence = derivative(fluxes[0], 1) + derivative(fluxes[1], 2) + derivative(fluxes[2], 3)
    return kernel_fields[0] * densities + kernel_fields[1] * aligned - divergence


def reference(occupied, virtual, kernel_fields, density_grad):
    def pair_block(orbital):
        return respond(orbital[None] * virtual, kernel_fields, density_grad)

    potential = lax.map(pair_block, occupied).reshape((NOCC * NVIR, NX, NY, NZ))
    flat_potential = potential.reshape((NOCC * NVIR, NX * NY * NZ))

    def rows_of(orbital):
        densities = (orbital[None] * virtual).reshape((NVIR, NX * NY * NZ))
        return lax.dot_general(densities, flat_potential, (((1,), (1,)), ((), ())), precision=lax.Precision.HIGHEST, preferred_element_type=jnp.float32)

    casida = lax.map(rows_of, occupied).reshape((NOCC * NVIR, NOCC * NVIR)) * (1.0 / (NX * NY * NZ))
    return potential, casida
```

```python
import functools

import jax
import jax.numpy as jnp
from jax import lax
from jax.experimental import pallas as pl
from jax.experimental.pallas import tpu as pltpu
from jax.sharding import PartitionSpec as P

MESH = pl.DeviceIdType.MESH
F32 = jnp.float32
BF16 = jnp.bfloat16
SHIFTS = (1, -1, 2, -2)


def rolled(value, shift):
    shift %= 128
    return value if shift == 0 else pltpu.roll(value, shift, value.ndim - 1)


def lanes(rows):
    return lax.broadcasted_iota(jnp.int32, (rows, 128), 1)


def stencil(plus1, minus1, plus2, minus2):
    return 8.0 * (plus1 - minus1) - (plus2 - minus2)


def split_halves(value):
    high = value.astype(BF16)
    return high, (value - high.astype(F32)).astype(BF16)


def columns_of(x):
    return range(-2, 6) if 0 <= x < 4 else range(4)


def kernel(
    sizes, scale,
    occ, vir, kf, dg,
    pot_out, cas_out,
    ext, own, cxo, cxl, cxr, cyo, cyhi, cylo, cyl, cyr,
    opk, zl, zr, hpk, hxl, hxr, hyl, hyr, czh, epk,
    nbuf, fxb, fyb, fzb, potb, dh, dl, ph, plow,
    cas, ra, dbuf, rb,
    send, recv, asend, arecv, bsend, brecv, osem,
):
    ngx, ngy, ngz = sizes
    gx, gy, gz = lax.axis_index("gx"), lax.axis_index("gy"), lax.axis_index("gz")

    def device(dx=0, dy=0, dz=0):
        return {
            "gx": lax.rem(gx + dx + ngx, ngx),
            "gy": lax.rem(gy + dy + ngy, ngy),
            "gz": lax.rem(gz + dz + ngz, ngz),
        }

    nb = ngy * ngz
    barrier = pltpu.get_barrier_semaphore()
    for k in range(1, ngx):
        pl.semaphore_signal(barrier, inc=1, device_id=device(dx=k), device_id_type=MESH)
    for k in range(1, nb):
        pl.semaphore_signal(
            barrier, inc=1, device_id=device(dy=k // ngz, dz=k % ngz), device_id_type=MESH
        )

    for c in range(16):
        x, y = divmod(c, 4)
        ext[4 + x, 4 + y, 0:16, :] = occ[pl.ds(c, 16, stride=16), :]
        ext[4 + x, 4 + y, 16:32, :] = vir[pl.ds(c, 16, stride=16), :]

    f0, f1, f2, f3 = (kf[pl.ds(16 * k, 16), :] for k in range(4))
    g = [dg[pl.ds(16 * k, 16), :] * (1.0 / 12.0) for k in range(3)]
    f3s = f3 * (1.0 / 144.0)
    for k, value in enumerate((f0, f1, f2, f3s, *g)):
        own[k] = value

    def combined(k):
        parts = [g[k] * f1]
        for other in range(3):
            beta = g[k] * g[other] * f2
            parts.append(beta + f3s if other == k else beta)
        return parts

    for k, value in enumerate(combined(0)):
        cxo[k] = value
    for k, value in enumerate(combined(1)):
        cyo[k] = value
    for k in range(4):
        cylo[k] = jnp.concatenate([cyo[k, 4 * x : 4 * x + 2, :] for x in range(4)], axis=0)
        cyhi[k] = jnp.concatenate([cyo[k, 4 * x + 2 : 4 * x + 4, :] for x in range(4)], axis=0)

    lane32 = lanes(32)

    def pack(at):
        total = None
        for c in range(16):
            part = rolled(at(c), 4 + 8 * c)
            total = part if total is None else jnp.where(lane32 // 8 == c, part, total)
        return total

    opk[0:32, :] = pack(lambda c: ext[4 + c // 4, 4 + c % 4])
    row16 = lax.broadcasted_iota(jnp.int32, (16, 128), 0)
    zrows = []
    for value in combined(2):
        turned = pltpu.roll(value, 4, 1, stride=8, stride_axis=0)
        zrows.append(
            jnp.sum(jnp.where(lanes(16) // 8 == row16, turned, 0.0), axis=0, keepdims=True)
        )
    opk[32:40, :] = jnp.concatenate(zrows + zrows, axis=0)

    pl.semaphore_wait(barrier, ngx - 1 + nb - 1)

    copies = {}

    def push(name, src, dst, target):
        k = len(copies)
        copies[name] = pltpu.make_async_remote_copy(
            src_ref=src, dst_ref=dst, send_sem=send.at[k], recv_sem=recv.at[k],
            device_id=target, device_id_type=MESH,
        )
        copies[name].start()

    push("zl", opk, zl, device(dz=1))
    push("zr", opk, zr, device(dz=-1))
    block = ext.at[4:8, 4:8]
    push("cyl", cyhi, cyl, device(dy=1))
    push("cyr", cylo, cyr, device(dy=-1))
    push("yl", block, ext.at[4:8, 0:4], device(dy=1))
    push("yr", block, ext.at[4:8, 8:12], device(dy=-1))
    push("cxl", cxo.at[:, 8:16], cxl, device(dx=1))
    push("cxr", cxo.at[:, 0:8], cxr, device(dx=-1))
    push("xl", block, ext.at[0:4, 4:8], device(dx=1))
    push("xr", block, ext.at[8:12, 4:8], device(dx=-1))

    def arrived(*names):
        for name in names:
            copies[name].wait_recv()

    arrived("zl", "zr")
    inner32 = lane32 % 8 < 4
    hpk[...] = jnp.where(inner32, zl[0:32, :], zr[0:32, :])
    czh[...] = jnp.where(lanes(8) % 8 < 4, zl[32:40, :], zr[32:40, :])
    push("hyl", hpk, hyl, device(dy=1))
    push("hyr", hpk, hyr, device(dy=-1))
    push("hxl", hpk, hxl, device(dx=1))
    push("hxr", hpk, hxr, device(dx=-1))

    arrived("yl", "yr")
    push("cll", ext.at[6:8, 2:4], ext.at[2:4, 2:4], device(dx=1))
    push("clr", ext.at[6:8, 8:10], ext.at[2:4, 8:10], device(dx=1))
    push("crl", ext.at[4:6, 2:4], ext.at[8:10, 2:4], device(dx=-1))
    push("crr", ext.at[4:6, 8:10], ext.at[8:10, 8:10], device(dx=-1))
    arrived("xl", "xr", "hyl", "hyr", "hxl", "hxr", "cyl", "cyr", "cxl", "cxr")
    arrived("cll", "clr", "crl", "crr")

    def edges(at, opack, hpack):
        high = jnp.where(inner32, opack, hpack)
        low = jnp.where(inner32, hpack, opack)
        for k, s in enumerate(SHIFTS):
            epk[at + k] = jnp.where(inner32, rolled(high, -s), rolled(low, -s))
        return high, low

    halo = hpk[...]
    high, low = edges(0, opk[0:32, :], halo)
    xpack = pack(lambda c: ext[(8 if c // 4 < 2 else 0) + c // 4, 4 + c % 4])
    edges(4, xpack, jnp.where(lane32 < 64, hxr[...], hxl[...]))
    ypack = pack(lambda c: ext[4 + c // 4, (8 if c % 4 < 2 else 0) + c % 4])
    edges(8, ypack, jnp.where(lane32 % 32 < 16, hyr[...], hyl[...]))
    epk[12] = halo
    for k, s in enumerate(SHIFTS):
        side_x, side_y = (hxr, hyr) if s > 0 else (hxl, hyl)
        inside_x = lane32 < 128 - 32 * s if s > 0 else lane32 >= -32 * s
        inside_y = lane32 % 32 < 32 - 8 * s if s > 0 else lane32 % 32 >= -8 * s
        epk[13 + k] = jnp.where(inside_x, rolled(halo, -32 * s), rolled(side_x[...], -32 * s))
        over = 32 - 8 * s if s > 0 else -32 - 8 * s
        epk[17 + k] = jnp.where(inside_y, rolled(halo, -8 * s), rolled(side_y[...], over))
        epk[21 + k] = jnp.where(inner32, rolled(low, -s), rolled(high, -s))

    lane16 = lanes(16)
    rim = (lane16 < 2) | (lane16 >= 126)

    def wide(row):
        return jnp.broadcast_to(row, (16, 128))

    def per_orbital(i, carry):
        def packed(k):
            return wide(epk[k, pl.ds(i, 1), :]) * epk[k, 16:32, :]

        def packed_slope(at):
            return stencil(*(packed(at + k) for k in range(4)))

        rims = [packed_slope(4 * k) for k in range(3)]
        zedge = (
            wide(czh[0:1, :]) * packed(12)
            + wide(czh[1:2, :]) * packed_slope(13)
            + wide(czh[2:3, :]) * packed_slope(17)
            + wide(czh[3:4, :]) * packed_slope(21)
        )

        for x in range(-4, 8):
            if 0 <= x < 4:
                ys = range(-4, 8)
            elif -2 <= x < 6:
                ys = range(-2, 6)
            else:
                ys = range(4)
            for y in ys:
                at = (4 + x, 4 + y)
                nbuf[at[0], at[1]] = wide(ext[at[0], at[1], pl.ds(i, 1), :]) * ext[at[0], at[1], 16:32, :]

        for x in range(-2, 6):
            inside = 0 <= x < 4
            line = {y: nbuf[4 + x, 4 + y] for y in (range(-4, 8) if inside else range(-2, 6))}
            for y in columns_of(x):
                n = line[y]
                sx = stencil(*(nbuf[4 + x + s, 4 + y] for s in SHIFTS))
                sy = stencil(*(line[y + s] for s in SHIFTS))
                sz = stencil(*(rolled(n, -s) for s in SHIFTS))
                c = (x % 4) * 4 + y % 4
                kind = 1 if not inside else (2 if not 0 <= y < 4 else 0)
                sz = jnp.where(rim, rolled(rims[kind], 124 - 8 * c), sz)
                if kind == 0:
                    f0, f1, f2, f3, g0, g1, g2 = (wide(own[k, c : c + 1, :]) for k in range(7))
                    aligned = g0 * sx + g1 * sy + g2 * sz
                    scalar = f1 * n + f2 * aligned
                    fxb[x + 2, y] = scalar * g0 + f3 * sx
                    fyb[x, y + 2] = scalar * g1 + f3 * sy
                    fzb[c] = scalar * g2 + f3 * sz
                    potb[c, pl.ds(pl.multiple_of(i * 16, 16), 16), :] = f0 * n + f1 * aligned
                else:
                    if kind == 1:
                        ref, row = (cxl, (x + 2) * 4 + y) if x < 0 else (cxr, (x - 4) * 4 + y)
                    else:
                        ref, row = (cyl, x * 2 + y + 2) if y < 0 else (cyr, x * 2 + y - 4)
                    c0, c1, c2, c3 = (wide(ref[k, row : row + 1, :]) for k in range(4))
                    flux = c0 * n + c1 * sx + c2 * sy + c3 * sz
                    if kind == 1:
                        fxb[x + 2, y] = flux
                    else:
                        fyb[x, y + 2] = flux

        rows = pl.ds(pl.multiple_of(i * 16, 16), 16)
        for c in range(16):
            x, y = divmod(c, 4)
            dx = stencil(*(fxb[x + 2 + s, y] for s in SHIFTS))
            dy = stencil(*(fyb[x, y + 2 + s] for s in SHIFTS))
            flux = fzb[c]
            near = []
            for s in SHIFTS:
                beyond = lane16 >= 128 - s if s > 0 else lane16 < -s
                over = (124 - s if s > 0 else 124 - s) - 8 * c
                near.append(jnp.where(beyond, rolled(zedge, over), rolled(flux, -s)))
            dz = stencil(*near)
            value = potb[c, rows, :] - (dx + dy + dz)
            potb[c, rows, :] = value
            high, low = split_halves(value)
            ph[rows, 128 * c : 128 * c + 128] = high
            plow[rows, 128 * c : 128 * c + 128] = low
            high, low = split_halves(nbuf[4 + x, 4 + y])
            dh[rows, 128 * c : 128 * c + 128] = high
            dl[rows, 128 * c : 128 * c + 128] = low
        pltpu.make_async_copy(potb.at[:, rows, :], pot_out.at[:, rows, :], osem.at[i]).start()
        return carry

    lax.fori_loop(0, 16, per_orbital, 0)

    def product(a, b):
        return lax.dot_general(a[...], b[...], (((1,), (1,)), ((), ())), preferred_element_type=F32)

    sums = (product(dh, ph) + product(dh, plow) + product(dl, ph)) * scale
    for k in range(ngx):
        cas[k] = sums[nb * k : nb * (k + 1), :]

    first = []
    for k in range(1, ngx):
        copy = pltpu.make_async_remote_copy(
            src_ref=cas.at[lax.rem(gx + k, ngx)], dst_ref=ra.at[k],
            send_sem=asend.at[k], recv_sem=arecv.at[k],
            device_id=device(dx=k), device_id_type=MESH,
        )
        copy.start()
        first.append(copy)
    for copy in first:
        copy.wait_recv()
    part = cas[gx]
    for k in range(1, ngx):
        part = part + ra[k]
    for r in range(nb):
        dbuf[r] = part[r : r + 1, :]
    second = []
    for k in range(1, nb):
        dy, dz = k // ngz, k % ngz
        there = device(dy=dy, dz=dz)
        copy = pltpu.make_async_remote_copy(
            src_ref=dbuf.at[there["gy"] * ngz + there["gz"]], dst_ref=rb.at[k],
            send_sem=bsend.at[k], recv_sem=brecv.at[k],
            device_id=there, device_id_type=MESH,
        )
        copy.start()
        second.append(copy)
    for copy in second:
        copy.wait_recv()
    row = dbuf[gy * ngz + gz]
    for k in range(1, nb):
        row = row + rb[k]
    cas_out[...] = row

    for copy in (*copies.values(), *first, *second):
        copy.wait_send()

    def drain(i, carry):
        rows = pl.ds(pl.multiple_of(i * 16, 16), 16)
        pltpu.make_async_copy(potb.at[:, rows, :], pot_out.at[:, rows, :], osem.at[i]).wait()
        return carry

    lax.fori_loop(0, 16, drain, 0)


def on_device(sizes, scale, occupied, virtual, kernel_fields, density_grad):
    ngx, ngy, ngz = sizes
    nb = ngy * ngz
    vmem = pltpu.VMEM
    dma = pltpu.SemaphoreType.DMA
    scratch = [
        vmem((12, 12, 32, 128), F32), vmem((7, 16, 128), F32),
        vmem((4, 16, 128), F32), vmem((4, 8, 128), F32), vmem((4, 8, 128), F32),
        vmem((4, 16, 128), F32), vmem((4, 8, 128), F32), vmem((4, 8, 128), F32),
        vmem((4, 8, 128), F32), vmem((4, 8, 128), F32),
        vmem((40, 128), F32), vmem((40, 128), F32), vmem((40, 128), F32),
        vmem((32, 128), F32), vmem((32, 128), F32), vmem((32, 128), F32),
        vmem((32, 128), F32), vmem((32, 128), F32), vmem((8, 128), F32),
        vmem((25, 32, 128), F32),
        vmem((12, 12, 16, 128), F32), vmem((8, 4, 16, 128), F32), vmem((4, 8, 16, 128), F32),
        vmem((16, 16, 128), F32), vmem((16, 256, 128), F32),
        vmem((256, 2048), BF16), vmem((256, 2048), BF16),
        vmem((256, 2048), BF16), vmem((256, 2048), BF16),
        vmem((ngx, nb, 256), F32), vmem((ngx, nb, 256), F32),
        vmem((nb, 1, 256), F32), vmem((nb, 1, 256), F32),
        dma((18,)), dma((18,)), dma((ngx,)), dma((ngx,)), dma((nb,)), dma((nb,)), dma((16,)),
    ]
    inner = pl.BlockSpec(memory_space=pltpu.VMEM)
    potential, row = pl.pallas_call(
        functools.partial(kernel, sizes, scale),
        out_shape=(
            jax.ShapeDtypeStruct((16, 256, 128), F32),
            jax.ShapeDtypeStruct((1, 256), F32),
        ),
        in_specs=[inner] * 4,
        out_specs=(pl.BlockSpec(memory_space=pl.ANY), inner),
        scratch_shapes=scratch,
        compiler_params=pltpu.CompilerParams(
            collective_id=0, has_side_effects=True, vmem_limit_bytes=48 * 1024 * 1024
        ),
    )(
        occupied.reshape(256, 128), virtual.reshape(256, 128),
        kernel_fields.reshape(64, 128), density_grad.reshape(48, 128),
    )
    return potential.transpose(1, 0, 2).reshape(256, 4, 4, 128), row


def solution(mesh):
    sizes = tuple(mesh.shape[axis] for axis in ("gx", "gy", "gz"))
    scale = 1.0 / (2048 * sizes[0] * sizes[1] * sizes[2])
    placed = P(None, "gx", "gy", "gz")
    return jax.shard_map(
        functools.partial(on_device, sizes, scale),
        mesh=mesh,
        in_specs=(placed,) * 4,
        out_specs=(placed, P(("gx", "gy", "gz"), None)),
        check_vma=False,
    )
```

```python
import functools

import jax
import jax.numpy as jnp
from jax import lax
from jax.experimental import pallas as pl
from jax.experimental.pallas import tpu as pltpu
from jax.sharding import PartitionSpec as P

MESH = pl.DeviceIdType.MESH
F32 = jnp.float32
BF16 = jnp.bfloat16
SHIFTS = (1, -1, 2, -2)


def rolled(value, shift):
    shift %= 128
    return value if shift == 0 else pltpu.roll(value, shift, value.ndim - 1)


def lanes(rows):
    return lax.broadcasted_iota(jnp.int32, (rows, 128), 1)


def stencil(plus1, minus1, plus2, minus2):
    return 8.0 * (plus1 - minus1) - (plus2 - minus2)


def split_halves(value):
    high = value.astype(BF16)
    return high, (value - high.astype(F32)).astype(BF16)


def columns_of(x):
    return range(-2, 6) if 0 <= x < 4 else range(4)


def kernel(
    sizes, scale,
    occ_in, vir_in, kf_in, dg_in,
    pot, cas_out,
    occ, vir, kf, dg,
    ext, own, cxo, cxl, cxr, cyo, cyhi, cylo, cyl, cyr,
    opk, zl, zr, hpk, hxl, hxr, hyl, hyr, czh, epk,
    nall, nbuf, fxb, fyb, fzb, lh, ll, rh, rl, acc,
    cas, ra, dbuf, rb,
    send, recv, asend, arecv, bsend, brecv, isem, rounds,
):
    ngx, ngy, ngz = sizes
    gx, gy, gz = lax.axis_index("gx"), lax.axis_index("gy"), lax.axis_index("gz")
    nb = ngy * ngz

    def device(dx=0, dy=0, dz=0):
        return {
            "gx": lax.rem(gx + dx + ngx, ngx),
            "gy": lax.rem(gy + dy + ngy, ngy),
            "gz": lax.rem(gz + dz + ngz, ngz),
        }

    def greet(semaphore, offsets):
        for dx, dy, dz in offsets:
            pl.semaphore_signal(
                semaphore, inc=1, device_id=device(dx, dy, dz), device_id_type=MESH
            )

    nearest = [(0, 0, 1), (0, 0, -1), (0, 1, 0), (0, -1, 0), (1, 0, 0), (-1, 0, 0)]
    second_round = [(2, 0, 0), (-2, 0, 0), (0, 0, 2), (0, 0, -2)]
    second_round += [(0, dy, dz) for dy in (1, -1) for dz in (1, -1)]
    third_round = [(0, 0, 2), (0, 0, -2)]
    barrier = pltpu.get_barrier_semaphore()
    greet(barrier, nearest)

    loads = [
        pltpu.make_async_copy(src, dst, isem.at[k])
        for k, (src, dst) in enumerate(((occ_in, occ), (vir_in, vir), (kf_in, kf), (dg_in, dg)))
    ]
    for load in loads:
        load.start()
    for load in loads:
        load.wait()

    for c in range(16):
        x, y = divmod(c, 4)
        ext[4 + x, 4 + y, 0:16, :] = occ[pl.ds(c, 16, stride=16), :]
        ext[4 + x, 4 + y, 16:32, :] = vir[pl.ds(c, 16, stride=16), :]

    f0, f1, f2, f3 = (kf[pl.ds(16 * k, 16), :] for k in range(4))
    g = [dg[pl.ds(16 * k, 16), :] * (1.0 / 12.0) for k in range(3)]
    f3s = f3 * (1.0 / 144.0)
    for k, value in enumerate((f0, f1, f2, f3s, *g)):
        own[k] = value

    def combined(k):
        parts = [g[k] * f1]
        for other in range(3):
            beta = g[k] * g[other] * f2
            parts.append(beta + f3s if other == k else beta)
        return parts

    lane32 = lanes(32)

    def pack(at):
        total = None
        for c in range(16):
            part = rolled(at(c), 4 + 8 * c)
            total = part if total is None else jnp.where(lane32 // 8 == c, part, total)
        return total

    opk[0:32, :] = pack(lambda c: ext[4 + c // 4, 4 + c % 4])
    row16 = lax.broadcasted_iota(jnp.int32, (16, 128), 0)
    zrows = []
    for value in combined(2):
        turned = pltpu.roll(value, 4, 1, stride=8, stride_axis=0)
        zrows.append(
            jnp.sum(jnp.where(lanes(16) // 8 == row16, turned, 0.0), axis=0, keepdims=True)
        )
    opk[32:40, :] = jnp.concatenate(zrows + zrows, axis=0)
    for k, value in enumerate(combined(0)):
        cxo[k] = value
    for k, value in enumerate(combined(1)):
        cyo[k] = value
    for k in range(4):
        cylo[k] = jnp.concatenate([cyo[k, 4 * x : 4 * x + 2, :] for x in range(4)], axis=0)
        cyhi[k] = jnp.concatenate([cyo[k, 4 * x + 2 : 4 * x + 4, :] for x in range(4)], axis=0)

    pl.semaphore_wait(barrier, len(nearest))
    greet(rounds.at[0], nearest)

    copies = {}

    def push(name, src, dst, target):
        k = len(copies)
        copies[name] = pltpu.make_async_remote_copy(
            src_ref=src, dst_ref=dst, send_sem=send.at[k], recv_sem=recv.at[k],
            device_id=target, device_id_type=MESH,
        )
        copies[name].start()

    def arrived(*names):
        for name in names:
            copies[name].wait_recv()

    push("zl", opk, zl, device(dz=1))
    push("zr", opk, zr, device(dz=-1))
    blocks = {"v": pl.ds(16, 16), "a": pl.ds(0, 8), "b": pl.ds(8, 8), "f": pl.ds(0, 32)}
    up, down, four = pl.ds(6, 2), pl.ds(4, 2), pl.ds(4, 4)

    def push_y(kind):
        rows = blocks[kind]
        near = kind != "f"
        src, dst = (up, pl.ds(2, 2)) if near else (down, pl.ds(0, 2))
        push("yl" + kind, ext.at[four, src, rows], ext.at[four, dst, rows], device(dy=1))
        src, dst = (down, pl.ds(8, 2)) if near else (up, pl.ds(10, 2))
        push("yr" + kind, ext.at[four, src, rows], ext.at[four, dst, rows], device(dy=-1))

    def push_x(kind):
        rows = blocks[kind]
        near = kind != "f"
        src, dst = (up, pl.ds(2, 2)) if near else (down, pl.ds(0, 2))
        push("xl" + kind, ext.at[src, four, rows], ext.at[dst, four, rows], device(dx=1))
        src, dst = (down, pl.ds(8, 2)) if near else (up, pl.ds(10, 2))
        push("xr" + kind, ext.at[src, four, rows], ext.at[dst, four, rows], device(dx=-1))

    for kind in "vab":
        push_y(kind)
        push_x(kind)
    push("cyl", cyhi, cyl, device(dy=1))
    push("cyr", cylo, cyr, device(dy=-1))
    push("cxl", cxo.at[:, 8:16], cxl, device(dx=1))
    push("cxr", cxo.at[:, 0:8], cxr, device(dx=-1))

    arrived("zl", "zr")
    inner32 = lane32 % 8 < 4
    hpk[...] = jnp.where(inner32, zl[0:32, :], zr[0:32, :])
    czh[...] = jnp.where(lanes(8) % 8 < 4, zl[32:40, :], zr[32:40, :])

    def edges(at, opack, hpack):
        high = jnp.where(inner32, opack, hpack)
        low = jnp.where(inner32, hpack, opack)
        for k, s in enumerate(SHIFTS):
            epk[at + k] = jnp.where(inner32, rolled(high, -s), rolled(low, -s))
        return high, low

    halo = hpk[...]
    high, low = edges(0, opk[0:32, :], halo)
    for k, s in enumerate(SHIFTS):
        epk[21 + k] = jnp.where(inner32, rolled(low, -s), rolled(high, -s))
    epk[12] = halo

    push("hyl", hpk, hyl, device(dy=1))
    push("hyr", hpk, hyr, device(dy=-1))
    push("hxl", hpk, hxl, device(dx=1))
    push("hxr", hpk, hxr, device(dx=-1))
    push_y("f")
    push_x("f")

    pl.semaphore_wait(rounds.at[0], len(nearest))
    greet(rounds.at[1], second_round)

    lane16 = lanes(16)
    rim = (lane16 < 2) | (lane16 >= 126)

    def wide(row):
        return jnp.broadcast_to(row, (16, 128))

    def density(i, x, y):
        return wide(ext[4 + x, 4 + y, pl.ds(i, 1), :]) * ext[4 + x, 4 + y, 16:32, :]

    def packed(i, k):
        return wide(epk[k, pl.ds(i, 1), :]) * epk[k, 16:32, :]

    def packed_slope(i, at):
        return stencil(*(packed(i, at + k) for k in range(4)))

    def slope_z(n, rims, c):
        sz = stencil(*(rolled(n, -s) for s in SHIFTS))
        return jnp.where(rim, rolled(rims, 124 - 8 * c), sz)

    def corners():
        for name, src, dst, target in (
            ("cll", ext.at[up, pl.ds(2, 2)], ext.at[pl.ds(2, 2), pl.ds(2, 2)], 1),
            ("clr", ext.at[up, pl.ds(8, 2)], ext.at[pl.ds(2, 2), pl.ds(8, 2)], 1),
            ("crl", ext.at[down, pl.ds(2, 2)], ext.at[pl.ds(8, 2), pl.ds(2, 2)], -1),
            ("crr", ext.at[down, pl.ds(8, 2)], ext.at[pl.ds(8, 2), pl.ds(8, 2)], -1),
        ):
            push(name, src, dst, device(dx=target))

    arrived("ylv", "yrv", "xlv", "xrv", "yla", "yra", "xla", "xra")
    pl.semaphore_wait(rounds.at[1], len(second_round))
    greet(rounds.at[2], third_round)

    def first_pass(i, carry):
        rows = pl.ds(pl.multiple_of(i * 16, 16), 16)

        def keep(term, c, left, right):
            at = slice(128 * c, 128 * c + 128)
            lh[term, rows, at], ll[term, rows, at] = split_halves(left)
            rh[term, rows, at], rl[term, rows, at] = split_halves(right)

        rims = packed_slope(i, 0)
        for x in range(-2, 6):
            for y in columns_of(x):
                nall[i, x + 2, y + 2] = density(i, x, y)
        for x in range(4):
            line = {y: nall[i, x + 2, y + 2] for y in range(-2, 6)}
            for y in range(4):
                n = line[y]
                c = 4 * x + y
                sx = stencil(*(nall[i, x + 2 + s, y + 2] for s in SHIFTS))
                sy = stencil(*(line[y + s] for s in SHIFTS))
                sz = slope_z(n, rims, c)
                f0, f1, f2, f3, g0, g1, g2 = (wide(own[k, c : c + 1, :]) for k in range(7))
                aligned = g0 * sx + g1 * sy + g2 * sz
                scalar = f1 * n + f2 * aligned
                flux = scalar * g0 + f3 * sx
                fxb[i, x + 2, y] = flux
                keep(1, c, sx, flux)
                flux = scalar * g1 + f3 * sy
                fyb[i, x, y + 2] = flux
                keep(2, c, sy, flux)
                flux = scalar * g2 + f3 * sz
                fzb[i, c] = flux
                keep(3, c, sz, flux)
                local = f0 * n + f1 * aligned
                pot[c, rows, :] = local
                keep(0, c, n, local)
        return carry

    lax.fori_loop(0, 8, first_pass, 0)
    arrived("ylb", "yrb", "xlb", "xrb")
    corners()
    lax.fori_loop(8, 16, first_pass, 0)

    def product(a, b):
        return lax.dot_general(a, b, (((1,), (1,)), ((), ())), preferred_element_type=F32)

    acc[...] = jnp.zeros_like(acc)

    def multiply(t, carry):
        acc[...] += product(lh[t], rh[t]) + product(lh[t], rl[t]) + product(ll[t], rh[t])
        return carry

    lax.fori_loop(0, 4, multiply, 0)
    for k in range(ngx):
        cas[k] = acc[nb * k : nb * (k + 1), :] * scale

    pl.semaphore_wait(rounds.at[2], len(third_round))
    first = []
    for k in range(1, ngx):
        copy = pltpu.make_async_remote_copy(
            src_ref=cas.at[lax.rem(gx + k, ngx)], dst_ref=ra.at[k],
            send_sem=asend.at[k], recv_sem=arecv.at[k],
            device_id=device(dx=k), device_id_type=MESH,
        )
        copy.start()
        first.append(copy)
    second = []
    for k in range(1, nb):
        there = device(dy=k // ngz, dz=k % ngz)
        second.append(
            pltpu.make_async_remote_copy(
                src_ref=dbuf.at[there["gy"] * ngz + there["gz"]], dst_ref=rb.at[k],
                send_sem=bsend.at[k], recv_sem=brecv.at[k],
                device_id=there, device_id_type=MESH,
            )
        )

    def reduce_first():
        for copy in first:
            copy.wait_recv()
        part = cas[gx]
        for k in range(1, ngx):
            part = part + ra[k]
        for r in range(nb):
            dbuf[r] = part[r : r + 1, :]
        for copy in second:
            copy.start()

    arrived("xlf", "xrf", "ylf", "yrf", "hyl", "hyr", "hxl", "hxr", "cyl", "cyr", "cxl", "cxr")
    arrived("cll", "clr", "crl", "crr")
    xpack = pack(lambda c: ext[(8 if c // 4 < 2 else 0) + c // 4, 4 + c % 4])
    edges(4, xpack, jnp.where(lane32 < 64, hxr[...], hxl[...]))
    ypack = pack(lambda c: ext[4 + c // 4, (8 if c % 4 < 2 else 0) + c % 4])
    edges(8, ypack, jnp.where(lane32 % 32 < 16, hyr[...], hyl[...]))
    halo = hpk[...]
    for k, s in enumerate(SHIFTS):
        side_x, side_y = (hxr, hyr) if s > 0 else (hxl, hyl)
        inside_x = lane32 < 128 - 32 * s if s > 0 else lane32 >= -32 * s
        inside_y = lane32 % 32 < 32 - 8 * s if s > 0 else lane32 % 32 >= -8 * s
        epk[13 + k] = jnp.where(inside_x, rolled(halo, -32 * s), rolled(side_x[...], -32 * s))
        over = 32 - 8 * s if s > 0 else -32 - 8 * s
        epk[17 + k] = jnp.where(inside_y, rolled(halo, -8 * s), rolled(side_y[...], over))

    def second_pass(i, carry):
        rows = pl.ds(pl.multiple_of(i * 16, 16), 16)

        def at(x, y):
            if (0 <= x < 4 and -2 <= y < 6) or (0 <= y < 4 and -2 <= x < 6):
                return nall[i, x + 2, y + 2]
            return nbuf[x + 4, y + 4]

        rims = {4: packed_slope(i, 4), 8: packed_slope(i, 8)}
        zedge = (
            wide(czh[0:1, :]) * packed(i, 12)
            + wide(czh[1:2, :]) * packed_slope(i, 13)
            + wide(czh[2:3, :]) * packed_slope(i, 17)
            + wide(czh[3:4, :]) * packed_slope(i, 21)
        )
        for x in (-4, -3, -2, -1, 0, 1, 2, 3, 4, 5, 6, 7):
            if 0 <= x < 4:
                ys = (-4, -3, 6, 7)
            elif -2 <= x < 6:
                ys = (-2, -1, 4, 5)
            else:
                ys = (0, 1, 2, 3)
            for y in ys:
                nbuf[4 + x, 4 + y] = density(i, x, y)

        def halo_flux(x, y, refs, row, at_pack):
            n = at(x, y)
            sx = stencil(*(at(x + s, y) for s in SHIFTS))
            sy = stencil(*(at(x, y + s) for s in SHIFTS))
            sz = slope_z(n, rims[at_pack], (x % 4) * 4 + y % 4)
            c0, c1, c2, c3 = (wide(refs[k, row : row + 1, :]) for k in range(4))
            return c0 * n + c1 * sx + c2 * sy + c3 * sz

        for x in (-2, -1, 4, 5):
            for y in range(4):
                refs, row = (cxl, (x + 2) * 4 + y) if x < 0 else (cxr, (x - 4) * 4 + y)
                fxb[i, x + 2, y] = halo_flux(x, y, refs, row, 4)
        for x in range(4):
            for y in (-2, -1, 4, 5):
                refs, row = (cyl, x * 2 + y + 2) if y < 0 else (cyr, x * 2 + y - 4)
                fyb[i, x, y + 2] = halo_flux(x, y, refs, row, 8)

        for c in range(16):
            x, y = divmod(c, 4)
            dx = stencil(*(fxb[i, x + 2 + s, y] for s in SHIFTS))
            dy = stencil(*(fyb[i, x, y + 2 + s] for s in SHIFTS))
            flux = fzb[i, c]
            near = []
            for s in SHIFTS:
                beyond = lane16 >= 128 - s if s > 0 else lane16 < -s
                near.append(jnp.where(beyond, rolled(zedge, 124 - s - 8 * c), rolled(flux, -s)))
            dz = stencil(*near)
            pot[c, rows, :] = pot[c, rows, :] - (dx + dy + dz)
        return carry

    lax.fori_loop(0, 8, second_pass, 0)
    reduce_first()
    lax.fori_loop(8, 16, second_pass, 0)

    for copy in second:
        copy.wait_recv()
    row = dbuf[gy * ngz + gz]
    for k in range(1, nb):
        row = row + rb[k]
    cas_out[...] = row
    for copy in (*copies.values(), *first, *second):
        copy.wait_send()


def on_device(sizes, scale, occupied, virtual, kernel_fields, density_grad):
    ngx, ngy, ngz = sizes
    nb = ngy * ngz
    vmem = pltpu.VMEM
    dma = pltpu.SemaphoreType.DMA
    scratch = [
        vmem((256, 128), F32), vmem((256, 128), F32), vmem((64, 128), F32), vmem((48, 128), F32),
        vmem((12, 12, 32, 128), F32), vmem((7, 16, 128), F32),
        vmem((4, 16, 128), F32), vmem((4, 8, 128), F32), vmem((4, 8, 128), F32),
        vmem((4, 16, 128), F32), vmem((4, 8, 128), F32), vmem((4, 8, 128), F32),
        vmem((4, 8, 128), F32), vmem((4, 8, 128), F32),
        vmem((40, 128), F32), vmem((40, 128), F32), vmem((40, 128), F32),
        vmem((32, 128), F32), vmem((32, 128), F32), vmem((32, 128), F32),
        vmem((32, 128), F32), vmem((32, 128), F32), vmem((8, 128), F32),
        vmem((25, 32, 128), F32),
        vmem((16, 8, 8, 16, 128), F32), vmem((12, 12, 16, 128), F32),
        vmem((16, 8, 4, 16, 128), F32), vmem((16, 4, 8, 16, 128), F32), vmem((16, 16, 16, 128), F32),
        vmem((4, 256, 2048), BF16), vmem((4, 256, 2048), BF16),
        vmem((4, 256, 2048), BF16), vmem((4, 256, 2048), BF16), vmem((256, 256), F32),
        vmem((ngx, nb, 256), F32), vmem((ngx, nb, 256), F32),
        vmem((nb, 1, 256), F32), vmem((nb, 1, 256), F32),
        dma((32,)), dma((32,)), dma((ngx,)), dma((ngx,)), dma((nb,)), dma((nb,)), dma((4,)),
        pltpu.SemaphoreType.REGULAR((3,)),
    ]
    inner = pl.BlockSpec(memory_space=pltpu.VMEM)
    potential, row = pl.pallas_call(
        functools.partial(kernel, sizes, scale),
        out_shape=(
            jax.ShapeDtypeStruct((16, 256, 128), F32),
            jax.ShapeDtypeStruct((1, 256), F32),
        ),
        in_specs=[pl.BlockSpec(memory_space=pltpu.HBM)] * 4,
        out_specs=(inner, inner),
        scratch_shapes=scratch,
        compiler_params=pltpu.CompilerParams(
            collective_id=0, has_side_effects=True, vmem_limit_bytes=44 * 1024 * 1024
        ),
    )(
        occupied.reshape(256, 128), virtual.reshape(256, 128),
        kernel_fields.reshape(64, 128), density_grad.reshape(48, 128),
    )
    return potential.transpose(1, 0, 2).reshape(256, 4, 4, 128), row


def solution(mesh):
    sizes = tuple(mesh.shape[axis] for axis in ("gx", "gy", "gz"))
    scale = 1.0 / (2048 * sizes[0] * sizes[1] * sizes[2])
    placed = P(None, "gx", "gy", "gz")
    return jax.shard_map(
        functools.partial(on_device, sizes, scale),
        mesh=mesh,
        in_specs=(placed,) * 4,
        out_specs=(placed, P(("gx", "gy", "gz"), None)),
        check_vma=False,
    )
```

```python
import functools

import jax
import jax.numpy as jnp
from jax import lax
from jax.experimental import pallas as pl
from jax.experimental.pallas import tpu as pltpu
from jax.sharding import PartitionSpec as P

MESH = pl.DeviceIdType.MESH
F32 = jnp.float32
BF16 = jnp.bfloat16
SHIFTS = (1, -1, 2, -2)


def rolled(value, shift):
    shift %= 128
    return value if shift == 0 else pltpu.roll(value, shift, value.ndim - 1)


def lanes(rows):
    return lax.broadcasted_iota(jnp.int32, (rows, 128), 1)


def stencil(plus1, minus1, plus2, minus2):
    return 8.0 * (plus1 - minus1) - (plus2 - minus2)


def split_halves(value):
    high = value.astype(BF16)
    return high, (value - high.astype(F32)).astype(BF16)


def columns_of(x):
    return range(-2, 6) if 0 <= x < 4 else range(4)


def kernel(
    sizes, scale,
    everything,
    pot, cas_out,
    ext, own, cxo, cxl, cxr, cyo, cyhi, cylo, cyl, cyr,
    opk, zl, zr, hpk, hxl, hxr, hyl, hyr, czh, epk,
    nall, nbuf, fxb, fyb, fzb, local_pot, lh, ll, rh, rl, acc,
    cas, ra, dbuf, rb,
    send, recv, asend, arecv, bsend, brecv, rounds,
):
    ngx, ngy, ngz = sizes
    gx, gy, gz = lax.axis_index("gx"), lax.axis_index("gy"), lax.axis_index("gz")
    nb = ngy * ngz

    def device(dx=0, dy=0, dz=0):
        return {
            "gx": lax.rem(gx + dx + ngx, ngx),
            "gy": lax.rem(gy + dy + ngy, ngy),
            "gz": lax.rem(gz + dz + ngz, ngz),
        }

    def greet(semaphore, offsets):
        for dx, dy, dz in offsets:
            pl.semaphore_signal(
                semaphore, inc=1, device_id=device(dx, dy, dz), device_id_type=MESH
            )

    nearest = [(0, 0, 1), (0, 0, -1), (0, 1, 0), (0, -1, 0), (1, 0, 0), (-1, 0, 0)]
    second_round = [(2, 0, 0), (-2, 0, 0), (0, 0, 2), (0, 0, -2)]
    second_round += [(0, dy, dz) for dy in (1, -1) for dz in (1, -1)]
    third_round = [(0, 0, 2), (0, 0, -2)]
    barrier = pltpu.get_barrier_semaphore()
    greet(barrier, nearest)

    for c in range(16):
        x, y = divmod(c, 4)
        ext[4 + x, 4 + y, 0:16, :] = everything[pl.ds(c, 16, stride=16), :]
        ext[4 + x, 4 + y, 16:32, :] = everything[pl.ds(256 + c, 16, stride=16), :]

    f0, f1, f2, f3 = (everything[pl.ds(512 + 16 * k, 16), :] for k in range(4))
    g = [everything[pl.ds(576 + 16 * k, 16), :] * (1.0 / 12.0) for k in range(3)]
    f3s = f3 * (1.0 / 144.0)
    for k, value in enumerate((f0, f1, f2, f3s, *g)):
        own[k] = value

    def combined(k):
        parts = [g[k] * f1]
        for other in range(3):
            beta = g[k] * g[other] * f2
            parts.append(beta + f3s if other == k else beta)
        return parts

    lane32 = lanes(32)

    def pack(at):
        total = None
        for c in range(16):
            part = rolled(at(c), 4 + 8 * c)
            total = part if total is None else jnp.where(lane32 // 8 == c, part, total)
        return total

    opk[0:32, :] = pack(lambda c: ext[4 + c // 4, 4 + c % 4])
    row16 = lax.broadcasted_iota(jnp.int32, (16, 128), 0)
    zrows = []
    for value in combined(2):
        turned = pltpu.roll(value, 4, 1, stride=8, stride_axis=0)
        zrows.append(
            jnp.sum(jnp.where(lanes(16) // 8 == row16, turned, 0.0), axis=0, keepdims=True)
        )
    opk[32:40, :] = jnp.concatenate(zrows + zrows, axis=0)
    for k, value in enumerate(combined(0)):
        cxo[k] = value
    for k, value in enumerate(combined(1)):
        cyo[k] = value
    for k in range(4):
        cylo[k] = jnp.concatenate([cyo[k, 4 * x : 4 * x + 2, :] for x in range(4)], axis=0)
        cyhi[k] = jnp.concatenate([cyo[k, 4 * x + 2 : 4 * x + 4, :] for x in range(4)], axis=0)

    pl.semaphore_wait(barrier, len(nearest))
    greet(rounds.at[0], nearest)

    copies = {}

    def push(name, src, dst, target):
        k = len(copies)
        copies[name] = pltpu.make_async_remote_copy(
            src_ref=src, dst_ref=dst, send_sem=send.at[k], recv_sem=recv.at[k],
            device_id=target, device_id_type=MESH,
        )
        copies[name].start()

    def arrived(*names):
        for name in names:
            copies[name].wait_recv()

    push("zl", opk, zl, device(dz=1))
    push("zr", opk, zr, device(dz=-1))
    blocks = {"v": pl.ds(16, 16), "a": pl.ds(0, 8), "b": pl.ds(8, 8), "f": pl.ds(0, 32)}
    up, down, four = pl.ds(6, 2), pl.ds(4, 2), pl.ds(4, 4)

    def push_y(kind):
        rows = blocks[kind]
        near = kind != "f"
        src, dst = (up, pl.ds(2, 2)) if near else (down, pl.ds(0, 2))
        push("yl" + kind, ext.at[four, src, rows], ext.at[four, dst, rows], device(dy=1))
        src, dst = (down, pl.ds(8, 2)) if near else (up, pl.ds(10, 2))
        push("yr" + kind, ext.at[four, src, rows], ext.at[four, dst, rows], device(dy=-1))

    def push_x(kind):
        rows = blocks[kind]
        near = kind != "f"
        src, dst = (up, pl.ds(2, 2)) if near else (down, pl.ds(0, 2))
        push("xl" + kind, ext.at[src, four, rows], ext.at[dst, four, rows], device(dx=1))
        src, dst = (down, pl.ds(8, 2)) if near else (up, pl.ds(10, 2))
        push("xr" + kind, ext.at[src, four, rows], ext.at[dst, four, rows], device(dx=-1))

    for kind in "vab":
        push_y(kind)
        push_x(kind)
    push("cyl", cyhi, cyl, device(dy=1))
    push("cyr", cylo, cyr, device(dy=-1))
    push("cxl", cxo.at[:, 8:16], cxl, device(dx=1))
    push("cxr", cxo.at[:, 0:8], cxr, device(dx=-1))

    arrived("zl", "zr")
    inner32 = lane32 % 8 < 4
    hpk[...] = jnp.where(inner32, zl[0:32, :], zr[0:32, :])
    czh[...] = jnp.where(lanes(8) % 8 < 4, zl[32:40, :], zr[32:40, :])

    def edges(at, opack, hpack):
        high = jnp.where(inner32, opack, hpack)
        low = jnp.where(inner32, hpack, opack)
        for k, s in enumerate(SHIFTS):
            epk[at + k] = jnp.where(inner32, rolled(high, -s), rolled(low, -s))
        return high, low

    halo = hpk[...]
    high, low = edges(0, opk[0:32, :], halo)
    for k, s in enumerate(SHIFTS):
        epk[21 + k] = jnp.where(inner32, rolled(low, -s), rolled(high, -s))
    epk[12] = halo

    push("hyl", hpk, hyl, device(dy=1))
    push("hyr", hpk, hyr, device(dy=-1))
    push("hxl", hpk, hxl, device(dx=1))
    push("hxr", hpk, hxr, device(dx=-1))
    push_y("f")
    push_x("f")

    lane16 = lanes(16)
    rim = (lane16 < 2) | (lane16 >= 126)

    def wide(row):
        return jnp.broadcast_to(row, (16, 128))

    def density(i, x, y):
        return wide(ext[4 + x, 4 + y, pl.ds(i, 1), :]) * ext[4 + x, 4 + y, 16:32, :]

    def packed(i, k):
        return wide(epk[k, pl.ds(i, 1), :]) * epk[k, 16:32, :]

    def packed_slope(i, at):
        return stencil(*(packed(i, at + k) for k in range(4)))

    def slope_z(n, rims, c):
        sz = stencil(*(rolled(n, -s) for s in SHIFTS))
        return jnp.where(rim, rolled(rims, 124 - 8 * c), sz)

    def corners():
        for name, src, dst, target in (
            ("cll", ext.at[up, pl.ds(2, 2)], ext.at[pl.ds(2, 2), pl.ds(2, 2)], 1),
            ("clr", ext.at[up, pl.ds(8, 2)], ext.at[pl.ds(2, 2), pl.ds(8, 2)], 1),
            ("crl", ext.at[down, pl.ds(2, 2)], ext.at[pl.ds(8, 2), pl.ds(2, 2)], -1),
            ("crr", ext.at[down, pl.ds(8, 2)], ext.at[pl.ds(8, 2), pl.ds(8, 2)], -1),
        ):
            push(name, src, dst, device(dx=target))

    arrived("ylv", "yrv", "xlv", "xrv", "yla", "yra", "xla", "xra")
    pl.semaphore_wait(rounds.at[0], len(nearest))
    greet(rounds.at[1], second_round)

    def first_pass(i, carry):
        rows = pl.ds(pl.multiple_of(i * 16, 16), 16)

        def keep(term, c, left, right):
            lh[term, c, rows, :], ll[term, c, rows, :] = split_halves(left)
            rh[term, c, rows, :], rl[term, c, rows, :] = split_halves(right)

        rims = packed_slope(i, 0)
        for x in range(-2, 6):
            for y in columns_of(x):
                nall[i, x + 2, y + 2] = density(i, x, y)
        for x in range(4):
            line = {y: nall[i, x + 2, y + 2] for y in range(-2, 6)}
            for y in range(4):
                n = line[y]
                c = 4 * x + y
                sx = stencil(*(nall[i, x + 2 + s, y + 2] for s in SHIFTS))
                sy = stencil(*(line[y + s] for s in SHIFTS))
                sz = slope_z(n, rims, c)
                f0, f1, f2, f3, g0, g1, g2 = (wide(own[k, c : c + 1, :]) for k in range(7))
                aligned = g0 * sx + g1 * sy + g2 * sz
                scalar = f1 * n + f2 * aligned
                flux = scalar * g0 + f3 * sx
                fxb[i, x + 2, y] = flux
                keep(1, c, sx, flux)
                flux = scalar * g1 + f3 * sy
                fyb[i, x, y + 2] = flux
                keep(2, c, sy, flux)
                flux = scalar * g2 + f3 * sz
                fzb[i, c] = flux
                keep(3, c, sz, flux)
                local = f0 * n + f1 * aligned
                local_pot[i, c] = local
                keep(0, c, n, local)
        return carry

    lax.fori_loop(0, 8, first_pass, 0)
    arrived("ylb", "yrb", "xlb", "xrb")
    corners()
    pl.semaphore_wait(rounds.at[1], len(second_round))
    greet(rounds.at[2], third_round)
    lax.fori_loop(8, 16, first_pass, 0)

    def product(a, b):
        return lax.dot_general(a, b, (((1,), (1,)), ((), ())), preferred_element_type=F32)

    acc[...] = jnp.zeros_like(acc)

    def multiply(t, carry):
        a, b, c, d = (
            jnp.concatenate([ref[t, k] for k in range(16)], axis=1) for ref in (lh, ll, rh, rl)
        )
        acc[...] += product(a, c) + product(a, d) + product(b, c)
        return carry

    lax.fori_loop(0, 4, multiply, 0)
    for k in range(ngx):
        cas[k] = acc[nb * k : nb * (k + 1), :] * scale

    pl.semaphore_wait(rounds.at[2], len(third_round))
    first = []
    for k in range(1, ngx):
        copy = pltpu.make_async_remote_copy(
            src_ref=cas.at[lax.rem(gx + k, ngx)], dst_ref=ra.at[k],
            send_sem=asend.at[k], recv_sem=arecv.at[k],
            device_id=device(dx=k), device_id_type=MESH,
        )
        copy.start()
        first.append(copy)
    second = []
    for k in range(1, nb):
        there = device(dy=k // ngz, dz=k % ngz)
        second.append(
            pltpu.make_async_remote_copy(
                src_ref=dbuf.at[there["gy"] * ngz + there["gz"]], dst_ref=rb.at[k],
                send_sem=bsend.at[k], recv_sem=brecv.at[k],
                device_id=there, device_id_type=MESH,
            )
        )

    def reduce_first():
        for copy in first:
            copy.wait_recv()
        part = cas[gx]
        for k in range(1, ngx):
            part = part + ra[k]
        for r in range(nb):
            dbuf[r] = part[r : r + 1, :]
        for copy in second:
            copy.start()

    arrived("xlf", "xrf", "ylf", "yrf", "hyl", "hyr", "hxl", "hxr", "cyl", "cyr", "cxl", "cxr")
    arrived("cll", "clr", "crl", "crr")
    xpack = pack(lambda c: ext[(8 if c // 4 < 2 else 0) + c // 4, 4 + c % 4])
    edges(4, xpack, jnp.where(lane32 < 64, hxr[...], hxl[...]))
    ypack = pack(lambda c: ext[4 + c // 4, (8 if c % 4 < 2 else 0) + c % 4])
    edges(8, ypack, jnp.where(lane32 % 32 < 16, hyr[...], hyl[...]))
    halo = hpk[...]
    for k, s in enumerate(SHIFTS):
        side_x, side_y = (hxr, hyr) if s > 0 else (hxl, hyl)
        inside_x = lane32 < 128 - 32 * s if s > 0 else lane32 >= -32 * s
        inside_y = lane32 % 32 < 32 - 8 * s if s > 0 else lane32 % 32 >= -8 * s
        epk[13 + k] = jnp.where(inside_x, rolled(halo, -32 * s), rolled(side_x[...], -32 * s))
        over = 32 - 8 * s if s > 0 else -32 - 8 * s
        epk[17 + k] = jnp.where(inside_y, rolled(halo, -8 * s), rolled(side_y[...], over))

    def second_pass(i, carry):
        def at(x, y):
            if (0 <= x < 4 and -2 <= y < 6) or (0 <= y < 4 and -2 <= x < 6):
                return nall[i, x + 2, y + 2]
            return nbuf[x + 4, y + 4]

        rims = {4: packed_slope(i, 4), 8: packed_slope(i, 8)}
        zedge = (
            wide(czh[0:1, :]) * packed(i, 12)
            + wide(czh[1:2, :]) * packed_slope(i, 13)
            + wide(czh[2:3, :]) * packed_slope(i, 17)
            + wide(czh[3:4, :]) * packed_slope(i, 21)
        )
        for x in (-4, -3, -2, -1, 0, 1, 2, 3, 4, 5, 6, 7):
            if 0 <= x < 4:
                ys = (-4, -3, 6, 7)
            elif -2 <= x < 6:
                ys = (-2, -1, 4, 5)
            else:
                ys = (0, 1, 2, 3)
            for y in ys:
                nbuf[4 + x, 4 + y] = density(i, x, y)

        def halo_flux(x, y, refs, row, at_pack):
            n = at(x, y)
            sx = stencil(*(at(x + s, y) for s in SHIFTS))
            sy = stencil(*(at(x, y + s) for s in SHIFTS))
            sz = slope_z(n, rims[at_pack], (x % 4) * 4 + y % 4)
            c0, c1, c2, c3 = (wide(refs[k, row : row + 1, :]) for k in range(4))
            return c0 * n + c1 * sx + c2 * sy + c3 * sz

        for x in (-2, -1, 4, 5):
            for y in range(4):
                refs, row = (cxl, (x + 2) * 4 + y) if x < 0 else (cxr, (x - 4) * 4 + y)
                fxb[i, x + 2, y] = halo_flux(x, y, refs, row, 4)
        for x in range(4):
            for y in (-2, -1, 4, 5):
                refs, row = (cyl, x * 2 + y + 2) if y < 0 else (cyr, x * 2 + y - 4)
                fyb[i, x, y + 2] = halo_flux(x, y, refs, row, 8)

        for c in range(16):
            x, y = divmod(c, 4)
            dx = stencil(*(fxb[i, x + 2 + s, y] for s in SHIFTS))
            dy = stencil(*(fyb[i, x, y + 2 + s] for s in SHIFTS))
            flux = fzb[i, c]
            near = []
            for s in SHIFTS:
                beyond = lane16 >= 128 - s if s > 0 else lane16 < -s
                near.append(jnp.where(beyond, rolled(zedge, 124 - s - 8 * c), rolled(flux, -s)))
            dz = stencil(*near)
            pot[pl.ds(i * 256 + c, 16, stride=16), :] = local_pot[i, c] - (dx + dy + dz)
        return carry

    lax.fori_loop(0, 6, second_pass, 0)
    reduce_first()
    lax.fori_loop(6, 16, second_pass, 0)

    for copy in second:
        copy.wait_recv()
    row = dbuf[gy * ngz + gz]
    for k in range(1, nb):
        row = row + rb[k]
    cas_out[...] = row
    for copy in (*copies.values(), *first, *second):
        copy.wait_send()


def on_device(sizes, scale, occupied, virtual, kernel_fields, density_grad):
    ngx, ngy, ngz = sizes
    nb = ngy * ngz
    vmem = pltpu.VMEM
    dma = pltpu.SemaphoreType.DMA
    scratch = [
        vmem((12, 12, 32, 128), F32), vmem((7, 16, 128), F32),
        vmem((4, 16, 128), F32), vmem((4, 8, 128), F32), vmem((4, 8, 128), F32),
        vmem((4, 16, 128), F32), vmem((4, 8, 128), F32), vmem((4, 8, 128), F32),
        vmem((4, 8, 128), F32), vmem((4, 8, 128), F32),
        vmem((40, 128), F32), vmem((40, 128), F32), vmem((40, 128), F32),
        vmem((32, 128), F32), vmem((32, 128), F32), vmem((32, 128), F32),
        vmem((32, 128), F32), vmem((32, 128), F32), vmem((8, 128), F32),
        vmem((25, 32, 128), F32),
        vmem((16, 8, 8, 16, 128), F32), vmem((12, 12, 16, 128), F32),
        vmem((16, 8, 4, 16, 128), F32), vmem((16, 4, 8, 16, 128), F32), vmem((16, 16, 16, 128), F32),
        vmem((16, 16, 16, 128), F32),
        vmem((4, 16, 256, 128), BF16), vmem((4, 16, 256, 128), BF16),
        vmem((4, 16, 256, 128), BF16), vmem((4, 16, 256, 128), BF16), vmem((256, 256), F32),
        vmem((ngx, nb, 256), F32), vmem((ngx, nb, 256), F32),
        vmem((nb, 1, 256), F32), vmem((nb, 1, 256), F32),
        dma((32,)), dma((32,)), dma((ngx,)), dma((ngx,)), dma((nb,)), dma((nb,)),
        pltpu.SemaphoreType.REGULAR((3,)),
    ]
    inner = pl.BlockSpec(memory_space=pltpu.VMEM)
    potential, row = pl.pallas_call(
        functools.partial(kernel, sizes, scale),
        out_shape=(
            jax.ShapeDtypeStruct((4096, 128), F32),
            jax.ShapeDtypeStruct((1, 256), F32),
        ),
        in_specs=[inner],
        out_specs=(inner, inner),
        scratch_shapes=scratch,
        compiler_params=pltpu.CompilerParams(
            collective_id=0, has_side_effects=True, vmem_limit_bytes=44 * 1024 * 1024
        ),
    )(jnp.concatenate([occupied, virtual, kernel_fields, density_grad], axis=0).reshape(624, 128))
    return potential.reshape(256, 4, 4, 128), row


def solution(mesh):
    sizes = tuple(mesh.shape[axis] for axis in ("gx", "gy", "gz"))
    scale = 1.0 / (2048 * sizes[0] * sizes[1] * sizes[2])
    placed = P(None, "gx", "gy", "gz")
    return jax.shard_map(
        functools.partial(on_device, sizes, scale),
        mesh=mesh,
        in_specs=(placed,) * 4,
        out_specs=(placed, P(("gx", "gy", "gz"), None)),
        check_vma=False,
    )
```

```python
import functools

import jax
import jax.numpy as jnp
from jax import lax
from jax.experimental import pallas as pl
from jax.experimental.pallas import tpu as pltpu
from jax.sharding import PartitionSpec as P

MESH = pl.DeviceIdType.MESH
F32 = jnp.float32
BF16 = jnp.bfloat16
SHIFTS = (1, -1, 2, -2)


def rolled(value, shift):
    shift %= 128
    return value if shift == 0 else pltpu.roll(value, shift, value.ndim - 1)


def lanes(rows):
    return lax.broadcasted_iota(jnp.int32, (rows, 128), 1)


def stencil(plus1, minus1, plus2, minus2):
    return 8.0 * (plus1 - minus1) - (plus2 - minus2)


def split_halves(value):
    high = value.astype(BF16)
    return high, (value - high.astype(F32)).astype(BF16)


def columns_of(x):
    return range(-2, 6) if 0 <= x < 4 else range(4)


def kernel(
    sizes, scale,
    everything,
    pot, cas_out,
    ext, own, cxo, cxl, cxr, cyo, cyhi, cylo, cyl, cyr,
    opk, zl, zr, hpk, hxl, hxr, hyl, hyr, czh, epk,
    nall, nbuf, sxb, szb, fzp, shifted, halo_coef, fxb, fyb, fzb, local_pot, lf, rf,
    cas, ra, dbuf, rb,
    send, recv, asend, arecv, bsend, brecv, rounds,
):
    ngx, ngy, ngz = sizes
    gx, gy, gz = lax.axis_index("gx"), lax.axis_index("gy"), lax.axis_index("gz")
    nb = ngy * ngz

    def device(dx=0, dy=0, dz=0):
        return {
            "gx": lax.rem(gx + dx + ngx, ngx),
            "gy": lax.rem(gy + dy + ngy, ngy),
            "gz": lax.rem(gz + dz + ngz, ngz),
        }

    def greet(semaphore, offsets):
        for dx, dy, dz in offsets:
            pl.semaphore_signal(
                semaphore, inc=1, device_id=device(dx, dy, dz), device_id_type=MESH
            )

    nearest = [(0, 0, 1), (0, 0, -1), (0, 1, 0), (0, -1, 0), (1, 0, 0), (-1, 0, 0)]
    second_round = [(2, 0, 0), (-2, 0, 0), (0, 0, 2), (0, 0, -2)]
    second_round += [(0, dy, dz) for dy in (1, -1) for dz in (1, -1)]
    third_round = [(0, 0, 2), (0, 0, -2)]
    barrier = pltpu.get_barrier_semaphore()
    greet(barrier, nearest)

    for c in range(16):
        x, y = divmod(c, 4)
        ext[4 + x, 4 + y, 0:16, :] = everything[pl.ds(c, 16, stride=16), :]
        ext[4 + x, 4 + y, 16:32, :] = everything[pl.ds(256 + c, 16, stride=16), :]

    f0, f1, f2, f3 = (everything[pl.ds(512 + 16 * k, 16), :] for k in range(4))
    g = [everything[pl.ds(576 + 16 * k, 16), :] * (1.0 / 12.0) for k in range(3)]
    f3s = f3 * (1.0 / 144.0)
    for k, value in enumerate((f0, f1, f2, f3s, *g)):
        for c in range(16):
            own[k, c] = jnp.broadcast_to(value[c : c + 1, :], (8, 128))

    def combined(k):
        parts = [g[k] * f1]
        for other in range(3):
            beta = g[k] * g[other] * f2
            parts.append(beta + f3s if other == k else beta)
        return parts

    lane32 = lanes(32)

    def pack(at):
        total = None
        for c in range(16):
            part = rolled(at(c), 4 + 8 * c)
            total = part if total is None else jnp.where(lane32 // 8 == c, part, total)
        return total

    opk[0:32, :] = pack(lambda c: ext[4 + c // 4, 4 + c % 4])
    row16 = lax.broadcasted_iota(jnp.int32, (16, 128), 0)
    zrows = []
    for value in combined(2):
        turned = pltpu.roll(value, 4, 1, stride=8, stride_axis=0)
        zrows.append(
            jnp.sum(jnp.where(lanes(16) // 8 == row16, turned, 0.0), axis=0, keepdims=True)
        )
    opk[32:40, :] = jnp.concatenate(zrows + zrows, axis=0)
    for k, value in enumerate(combined(0)):
        cxo[k] = value
    for k, value in enumerate(combined(1)):
        cyo[k] = value
    for k in range(4):
        cylo[k] = jnp.concatenate([cyo[k, 4 * x : 4 * x + 2, :] for x in range(4)], axis=0)
        cyhi[k] = jnp.concatenate([cyo[k, 4 * x + 2 : 4 * x + 4, :] for x in range(4)], axis=0)

    pl.semaphore_wait(barrier, len(nearest))
    greet(rounds.at[0], nearest)

    copies = {}

    def push(name, src, dst, target):
        k = len(copies)
        copies[name] = pltpu.make_async_remote_copy(
            src_ref=src, dst_ref=dst, send_sem=send.at[k], recv_sem=recv.at[k],
            device_id=target, device_id_type=MESH,
        )
        copies[name].start()

    def arrived(*names):
        for name in names:
            copies[name].wait_recv()

    push("zl", opk, zl, device(dz=1))
    push("zr", opk, zr, device(dz=-1))
    blocks = {"v": pl.ds(16, 16), "a": pl.ds(0, 4), "b": pl.ds(4, 4), "c": pl.ds(8, 8), "f": pl.ds(0, 32)}
    up, down, four = pl.ds(6, 2), pl.ds(4, 2), pl.ds(4, 4)

    def push_y(kind):
        rows = blocks[kind]
        near = kind != "f"
        src, dst = (up, pl.ds(2, 2)) if near else (down, pl.ds(0, 2))
        push("yl" + kind, ext.at[four, src, rows], ext.at[four, dst, rows], device(dy=1))
        src, dst = (down, pl.ds(8, 2)) if near else (up, pl.ds(10, 2))
        push("yr" + kind, ext.at[four, src, rows], ext.at[four, dst, rows], device(dy=-1))

    def push_x(kind):
        rows = blocks[kind]
        near = kind != "f"
        src, dst = (up, pl.ds(2, 2)) if near else (down, pl.ds(0, 2))
        push("xl" + kind, ext.at[src, four, rows], ext.at[dst, four, rows], device(dx=1))
        src, dst = (down, pl.ds(8, 2)) if near else (up, pl.ds(10, 2))
        push("xr" + kind, ext.at[src, four, rows], ext.at[dst, four, rows], device(dx=-1))

    for kind in "vabc":
        push_y(kind)
        push_x(kind)
    push("cyl", cyhi, cyl, device(dy=1))
    push("cyr", cylo, cyr, device(dy=-1))
    push("cxl", cxo.at[:, 8:16], cxl, device(dx=1))
    push("cxr", cxo.at[:, 0:8], cxr, device(dx=-1))

    lane16 = lanes(16)
    rim = (lane16 < 2) | (lane16 >= 126)
    rim32 = (lane32 < 2) | (lane32 >= 126)

    def wide(row):
        return jnp.broadcast_to(row, (16, 128))

    def twice(value):
        return jnp.concatenate([value, value], axis=0)

    def rows_of(i):
        return pl.ds(pl.multiple_of(i * 16, 16), 16)

    def density(i, x, y):
        return wide(ext[4 + x, 4 + y, pl.ds(i, 1), :]) * ext[4 + x, 4 + y, 16:32, :]

    def packed(i, k):
        return wide(epk[k, pl.ds(i, 1), :]) * epk[k, 16:32, :]

    def packed_slope(i, at):
        return stencil(*(packed(i, at + k) for k in range(4)))

    def slope_z(n, rims, c):
        sz = stencil(*(rolled(n, -s) for s in SHIFTS))
        return jnp.where(rim, rolled(rims, 124 - 8 * c), sz)

    def own_columns(i, carry):
        rows = rows_of(i)
        for c in range(16):
            x, y = divmod(c, 4)
            n = density(i, x, y)
            nall[i, x + 2, y + 2] = n
            szb[i, c] = stencil(*(rolled(n, -s) for s in SHIFTS))
            lf[0, c, 0, rows, :], lf[0, c, 1, rows, :] = split_halves(n)
        return carry

    lax.fori_loop(0, 16, own_columns, 0)

    arrived("zl", "zr")
    inner32 = lane32 % 8 < 4
    hpk[...] = jnp.where(inner32, zl[0:32, :], zr[0:32, :])
    czh[...] = jnp.where(lanes(8) % 8 < 4, zl[32:40, :], zr[32:40, :])

    def edges(at, opack, hpack):
        high = jnp.where(inner32, opack, hpack)
        low = jnp.where(inner32, hpack, opack)
        for k, s in enumerate(SHIFTS):
            epk[at + k] = jnp.where(inner32, rolled(high, -s), rolled(low, -s))
        return high, low

    halo = hpk[...]
    high, low = edges(0, opk[0:32, :], halo)
    for k, s in enumerate(SHIFTS):
        epk[21 + k] = jnp.where(inner32, rolled(low, -s), rolled(high, -s))
    epk[12] = halo

    push("hyl", hpk, hyl, device(dy=1))
    push("hyr", hpk, hyr, device(dy=-1))
    push("hxl", hpk, hxl, device(dx=1))
    push("hxr", hpk, hxr, device(dx=-1))
    push_y("f")
    push_x("f")

    def corners():
        for name, src, dst, target in (
            ("cll", ext.at[up, pl.ds(2, 2)], ext.at[pl.ds(2, 2), pl.ds(2, 2)], 1),
            ("clr", ext.at[up, pl.ds(8, 2)], ext.at[pl.ds(2, 2), pl.ds(8, 2)], 1),
            ("crl", ext.at[down, pl.ds(2, 2)], ext.at[pl.ds(8, 2), pl.ds(2, 2)], -1),
            ("crr", ext.at[down, pl.ds(8, 2)], ext.at[pl.ds(8, 2), pl.ds(8, 2)], -1),
        ):
            push(name, src, dst, device(dx=target))

    def coefficients(c, which):
        return (twice(own[k, c]) for k in which)

    def slopes_xz(i, carry):
        rows = rows_of(i)
        rims = packed_slope(i, 0)
        for y in range(4):
            line = {}
            for x in range(-2, 6):
                if 0 <= x < 4:
                    line[x] = nall[i, x + 2, y + 2]
                else:
                    line[x] = density(i, x, y)
                    nall[i, x + 2, y + 2] = line[x]
            for x in range(4):
                c = 4 * x + y
                sx = stencil(*(line[x + s] for s in SHIFTS))
                sz = jnp.where(rim, rolled(rims, 124 - 8 * c), szb[i, c])
                g0, g2 = coefficients(c, (4, 6))
                sxb[i, c] = sx
                szb[i, c] = sz
                local_pot[i, c] = g0 * sx + g2 * sz
                for term, value in ((1, sx), (3, sz)):
                    lf[term, c, 0, rows, :], lf[term, c, 1, rows, :] = split_halves(value)
        return carry

    arrived("xlv", "xrv", "xla", "xra", "xlb", "xrb", "xlc", "xrc")
    lax.fori_loop(0, 16, slopes_xz, 0)
    pl.semaphore_wait(rounds.at[0], len(nearest))
    greet(rounds.at[1], second_round)
    arrived("ylv", "yrv", "yla", "yra")

    def first_pass(i, carry):
        rows = rows_of(i)

        def keep(term, c, right):
            rf[term, c, 0, rows, :], rf[term, c, 1, rows, :] = split_halves(right)

        ends = None
        for x in range(4):
            line = {}
            for y in range(-2, 6):
                if 0 <= y < 4:
                    line[y] = nall[i, x + 2, y + 2]
                else:
                    line[y] = density(i, x, y)
                    nall[i, x + 2, y + 2] = line[y]
            for y in range(4):
                n = line[y]
                c = 4 * x + y
                sy = stencil(*(line[y + s] for s in SHIFTS))
                lf[2, c, 0, rows, :], lf[2, c, 1, rows, :] = split_halves(sy)
                f0, f1, f2, f3, g0, g1, g2 = coefficients(c, range(7))
                aligned = local_pot[i, c] + g1 * sy
                scalar = f1 * n + f2 * aligned
                flux = scalar * g0 + f3 * sxb[i, c]
                fxb[i, x + 2, y] = flux
                keep(1, c, flux)
                flux = scalar * g1 + f3 * sy
                fyb[i, x, y + 2] = flux
                keep(2, c, flux)
                flux = scalar * g2 + f3 * szb[i, c]
                fzb[i, c] = flux
                keep(3, c, flux)
                part = rolled(flux, 4 + 8 * c)
                ends = part if ends is None else jnp.where(lane16 // 8 == c, part, ends)
                local = f0 * n + f1 * aligned
                local_pot[i, c] = local
                keep(0, c, local)
        fzp[i] = ends
        return carry

    lax.fori_loop(0, 4, first_pass, 0)
    arrived("ylb", "yrb")
    lax.fori_loop(4, 8, first_pass, 0)
    arrived("ylc", "yrc")
    corners()
    pl.semaphore_wait(rounds.at[1], len(second_round))
    greet(rounds.at[2], third_round)
    lax.fori_loop(8, 16, first_pass, 0)

    def product(a, b):
        return lax.dot_general(a, b, (((1,), (1,)), ((), ())), preferred_element_type=F32)

    arrived("hyl", "hyr", "hxl", "hxr", "cyl", "cyr", "cxl", "cxr")
    sums = None
    for t in range(4):
        a, b, c, d = (
            jnp.concatenate([ref[t, k, half, 0:256, :] for k in range(16)], axis=1)
            for ref, half in ((lf, 0), (lf, 1), (rf, 0), (rf, 1))
        )
        part = product(a, c) + product(a, d) + product(b, c)
        sums = part if sums is None else sums + part

    xpack = pack(lambda c: ext[(8 if c // 4 < 2 else 0) + c // 4, 4 + c % 4])
    edges(4, xpack, jnp.where(lane32 < 64, hxr[...], hxl[...]))
    ypack = pack(lambda c: ext[4 + c // 4, (8 if c % 4 < 2 else 0) + c % 4])
    edges(8, ypack, jnp.where(lane32 % 32 < 16, hyr[...], hyl[...]))
    halo = hpk[...]
    for k, s in enumerate(SHIFTS):
        side_x, side_y = (hxr, hyr) if s > 0 else (hxl, hyl)
        inside_x = lane32 < 128 - 32 * s if s > 0 else lane32 >= -32 * s
        inside_y = lane32 % 32 < 32 - 8 * s if s > 0 else lane32 % 32 >= -8 * s
        epk[13 + k] = jnp.where(inside_x, rolled(halo, -32 * s), rolled(side_x[...], -32 * s))
        over = 32 - 8 * s if s > 0 else -32 - 8 * s
        epk[17 + k] = jnp.where(inside_y, rolled(halo, -8 * s), rolled(side_y[...], over))

    eights = jnp.where(lax.broadcasted_iota(jnp.int32, (32, 128), 0) < 16, 1.0, 8.0)
    halo_columns = [(x, y) for x in (-2, -1, 4, 5) for y in range(4)]
    for m, (x, y) in enumerate(halo_columns):
        c = (x % 4) * 4 + y % 4
        for k, s in enumerate(SHIFTS):
            value = ext[4 + x, 4 + y]
            edge = rolled(epk[4 + k], 124 - 8 * c)
            value = jnp.where(rim32, edge, rolled(value, -s))
            shifted[m, k] = value * eights if k < 2 else value

    for k in range(4):
        for r in range(8):
            for side, ref in enumerate((cxl, cxr, cyl, cyr)):
                halo_coef[k, side, r] = jnp.broadcast_to(ref[k, r : r + 1, :], (8, 128))
    for k in range(ngx):
        cas[k] = sums[nb * k : nb * (k + 1), :] * scale

    pl.semaphore_wait(rounds.at[2], len(third_round))
    first = []
    for k in range(1, ngx):
        copy = pltpu.make_async_remote_copy(
            src_ref=cas.at[lax.rem(gx + k, ngx)], dst_ref=ra.at[k],
            send_sem=asend.at[k], recv_sem=arecv.at[k],
            device_id=device(dx=k), device_id_type=MESH,
        )
        copy.start()
        first.append(copy)
    second = []
    for k in range(1, nb):
        there = device(dy=k // ngz, dz=k % ngz)
        second.append(
            pltpu.make_async_remote_copy(
                src_ref=dbuf.at[there["gy"] * ngz + there["gz"]], dst_ref=rb.at[k],
                send_sem=bsend.at[k], recv_sem=brecv.at[k],
                device_id=there, device_id_type=MESH,
            )
        )

    def reduce_first():
        for copy in first:
            copy.wait_recv()
        part = cas[gx]
        for k in range(1, ngx):
            part = part + ra[k]
        for r in range(nb):
            dbuf[r] = part[r : r + 1, :]
        for copy in second:
            copy.start()

    arrived("xlf", "xrf", "ylf", "yrf")
    arrived("cll", "clr", "crl", "crr")
    inner16 = lane16 % 8 < 4

    def second_pass(i, carry):
        def at(x, y):
            if (0 <= x < 4 and -2 <= y < 6) or (0 <= y < 4 and -2 <= x < 6):
                return nall[i, x + 2, y + 2]
            return nbuf[x + 4, y + 4]

        zedge = (
            wide(czh[0:1, :]) * packed(i, 12)
            + wide(czh[1:2, :]) * packed_slope(i, 13)
            + wide(czh[2:3, :]) * packed_slope(i, 17)
            + wide(czh[3:4, :]) * packed_slope(i, 21)
        )
        rims = packed_slope(i, 8)
        high = jnp.where(inner16, fzp[i], zedge)
        low = jnp.where(inner16, zedge, fzp[i])
        zends = stencil(*(jnp.where(inner16, rolled(high, -s), rolled(low, -s)) for s in SHIFTS))
        for x in (-4, -3, -2, -1, 0, 1, 2, 3, 4, 5, 6, 7):
            if 0 <= x < 4:
                ys = (-4, -3, 6, 7)
            elif -2 <= x < 6:
                ys = (-2, -1, 4, 5)
            else:
                ys = (0, 1, 2, 3)
            for y in ys:
                nbuf[4 + x, 4 + y] = density(i, x, y)

        def halo_flux(x, y, side, row, sz):
            n = at(x, y)
            sx = stencil(*(at(x + s, y) for s in SHIFTS))
            sy = stencil(*(at(x, y + s) for s in SHIFTS))
            c0, c1, c2, c3 = (twice(halo_coef[k, side, row]) for k in range(4))
            return c0 * n + c1 * sx + c2 * sy + c3 * sz

        for x in (-2, -1, 4, 5):
            for y in range(4):
                m = halo_columns.index((x, y))
                moved = [wide(shifted[m, k, pl.ds(i, 1), :]) * shifted[m, k, 16:32, :] for k in range(4)]
                sz = (moved[0] - moved[1]) - (moved[2] - moved[3])
                side, row = (0, (x + 2) * 4 + y) if x < 0 else (1, (x - 4) * 4 + y)
                fxb[i, x + 2, y] = halo_flux(x, y, side, row, sz)
        for x in range(4):
            for y in (-2, -1, 4, 5):
                sz = slope_z(at(x, y), rims, 4 * x + y % 4)
                side, row = (2, x * 2 + y + 2) if y < 0 else (3, x * 2 + y - 4)
                fyb[i, x, y + 2] = halo_flux(x, y, side, row, sz)

        for c in range(16):
            x, y = divmod(c, 4)
            dx = stencil(*(fxb[i, x + 2 + s, y] for s in SHIFTS))
            dy = stencil(*(fyb[i, x, y + 2 + s] for s in SHIFTS))
            flux = fzb[i, c]
            dz = stencil(*(rolled(flux, -s) for s in SHIFTS))
            dz = jnp.where(rim, rolled(zends, 124 - 8 * c), dz)
            pot[pl.ds(i * 256 + c, 16, stride=16), :] = local_pot[i, c] - (dx + dy + dz)
        return carry

    lax.fori_loop(0, 9, second_pass, 0)
    reduce_first()
    lax.fori_loop(9, 16, second_pass, 0)

    for copy in second:
        copy.wait_recv()
    row = dbuf[gy * ngz + gz]
    for k in range(1, nb):
        row = row + rb[k]
    cas_out[...] = row
    for copy in (*copies.values(), *first, *second):
        copy.wait_send()


def on_device(sizes, scale, occupied, virtual, kernel_fields, density_grad):
    ngx, ngy, ngz = sizes
    nb = ngy * ngz
    vmem = pltpu.VMEM
    dma = pltpu.SemaphoreType.DMA
    scratch = [
        vmem((12, 12, 32, 128), F32), vmem((7, 16, 8, 128), F32),
        vmem((4, 16, 128), F32), vmem((4, 8, 128), F32), vmem((4, 8, 128), F32),
        vmem((4, 16, 128), F32), vmem((4, 8, 128), F32), vmem((4, 8, 128), F32),
        vmem((4, 8, 128), F32), vmem((4, 8, 128), F32),
        vmem((40, 128), F32), vmem((40, 128), F32), vmem((40, 128), F32),
        vmem((32, 128), F32), vmem((32, 128), F32), vmem((32, 128), F32),
        vmem((32, 128), F32), vmem((32, 128), F32), vmem((8, 128), F32),
        vmem((25, 32, 128), F32),
        vmem((16, 8, 8, 16, 128), F32), vmem((12, 12, 16, 128), F32),
        vmem((16, 16, 16, 128), F32), vmem((16, 16, 16, 128), F32), vmem((16, 16, 128), F32),
        vmem((16, 4, 32, 128), F32), vmem((4, 4, 8, 8, 128), F32),
        vmem((16, 8, 4, 16, 128), F32), vmem((16, 4, 8, 16, 128), F32), vmem((16, 16, 16, 128), F32),
        vmem((16, 16, 16, 128), F32),
        vmem((4, 16, 2, 272, 128), BF16), vmem((4, 16, 2, 272, 128), BF16),
        vmem((ngx, nb, 256), F32), vmem((ngx, nb, 256), F32),
        vmem((nb, 1, 256), F32), vmem((nb, 1, 256), F32),
        dma((36,)), dma((36,)), dma((ngx,)), dma((ngx,)), dma((nb,)), dma((nb,)),
        pltpu.SemaphoreType.REGULAR((3,)),
    ]
    inner = pl.BlockSpec(memory_space=pltpu.VMEM)
    potential, row = pl.pallas_call(
        functools.partial(kernel, sizes, scale),
        out_shape=(
            jax.ShapeDtypeStruct((4096, 128), F32),
            jax.ShapeDtypeStruct((1, 256), F32),
        ),
        in_specs=[inner],
        out_specs=(inner, inner),
        scratch_shapes=scratch,
        compiler_params=pltpu.CompilerParams(
            collective_id=0, has_side_effects=True, vmem_limit_bytes=50 * 1024 * 1024
        ),
    )(jnp.concatenate([occupied, virtual, kernel_fields, density_grad], axis=0).reshape(624, 128))
    return potential.reshape(256, 4, 4, 128), row


def solution(mesh):
    sizes = tuple(mesh.shape[axis] for axis in ("gx", "gy", "gz"))
    scale = 1.0 / (2048 * sizes[0] * sizes[1] * sizes[2])
    placed = P(None, "gx", "gy", "gz")
    return jax.shard_map(
        functools.partial(on_device, sizes, scale),
        mesh=mesh,
        in_specs=(placed,) * 4,
        out_specs=(placed, P(("gx", "gy", "gz"), None)),
        check_vma=False,
    )
```

```python
import functools

import jax
import jax.numpy as jnp
from jax import lax
from jax.experimental import pallas as pl
from jax.experimental.pallas import tpu as pltpu
from jax.sharding import PartitionSpec as P

MESH = pl.DeviceIdType.MESH
F32 = jnp.float32
BF16 = jnp.bfloat16
SHIFTS = (1, -1, 2, -2)


def rolled(value, shift):
    shift %= 128
    return value if shift == 0 else pltpu.roll(value, shift, value.ndim - 1)


def lanes(rows):
    return lax.broadcasted_iota(jnp.int32, (rows, 128), 1)


def stencil(plus1, minus1, plus2, minus2):
    return 8.0 * (plus1 - minus1) - (plus2 - minus2)


def split_halves(value):
    high = value.astype(BF16)
    return high, (value - high.astype(F32)).astype(BF16)


def columns_of(x):
    return range(-2, 6) if 0 <= x < 4 else range(4)


def kernel(
    sizes, scale,
    everything,
    pot, cas_out,
    ext, own, cxo, cxl, cxr, cyo, cyhi, cylo, cyl, cyr,
    opk, zl, zr, hpk, hxl, hxr, hyl, hyr, czh, epk,
    nall, nbuf, szb, fzp, shifted, halo_coef, fxb, fyb, fzb, local_pot, lf, rf, ly, ry, acc,
    cas, ra, dbuf, rb,
    send, recv, asend, arecv, bsend, brecv, rounds,
):
    ngx, ngy, ngz = sizes
    gx, gy, gz = lax.axis_index("gx"), lax.axis_index("gy"), lax.axis_index("gz")
    nb = ngy * ngz

    def device(dx=0, dy=0, dz=0):
        return {
            "gx": lax.rem(gx + dx + ngx, ngx),
            "gy": lax.rem(gy + dy + ngy, ngy),
            "gz": lax.rem(gz + dz + ngz, ngz),
        }

    def greet(semaphore, offsets):
        for dx, dy, dz in offsets:
            pl.semaphore_signal(
                semaphore, inc=1, device_id=device(dx, dy, dz), device_id_type=MESH
            )

    nearest = [(0, 0, 1), (0, 0, -1), (0, 1, 0), (0, -1, 0), (1, 0, 0), (-1, 0, 0)]
    second_round = [(2, 0, 0), (-2, 0, 0), (0, 0, 2), (0, 0, -2)]
    second_round += [(0, dy, dz) for dy in (1, -1) for dz in (1, -1)]
    third_round = [(0, 0, 2), (0, 0, -2)]
    barrier = pltpu.get_barrier_semaphore()
    greet(barrier, nearest)

    for c in range(16):
        x, y = divmod(c, 4)
        ext[4 + x, 4 + y, 0:16, :] = everything[pl.ds(c, 16, stride=16), :]
        ext[4 + x, 4 + y, 16:32, :] = everything[pl.ds(256 + c, 16, stride=16), :]

    f0, f1, f2, f3 = (everything[pl.ds(512 + 16 * k, 16), :] for k in range(4))
    g = [everything[pl.ds(576 + 16 * k, 16), :] * (1.0 / 12.0) for k in range(3)]
    f3s = f3 * (1.0 / 144.0)
    crossed = (g[0] * g[1] * f2, g[1] * g[1] * f2 + f3s, g[2] * g[1] * f2, g[1] * f1)
    for k, value in enumerate((f0, f1, f2, f3s, *g, *crossed)):
        for c in range(16):
            own[k, c] = jnp.broadcast_to(value[c : c + 1, :], (8, 128))

    def combined(k):
        parts = [g[k] * f1]
        for other in range(3):
            beta = g[k] * g[other] * f2
            parts.append(beta + f3s if other == k else beta)
        return parts

    lane32 = lanes(32)

    def pack(at):
        total = None
        for c in range(16):
            part = rolled(at(c), 4 + 8 * c)
            total = part if total is None else jnp.where(lane32 // 8 == c, part, total)
        return total

    opk[0:32, :] = pack(lambda c: ext[4 + c // 4, 4 + c % 4])
    row16 = lax.broadcasted_iota(jnp.int32, (16, 128), 0)
    zrows = []
    for value in combined(2):
        turned = pltpu.roll(value, 4, 1, stride=8, stride_axis=0)
        zrows.append(
            jnp.sum(jnp.where(lanes(16) // 8 == row16, turned, 0.0), axis=0, keepdims=True)
        )
    opk[32:40, :] = jnp.concatenate(zrows + zrows, axis=0)
    for k, value in enumerate(combined(0)):
        cxo[k] = value
    for k, value in enumerate(combined(1)):
        cyo[k] = value
    for k in range(4):
        cylo[k] = jnp.concatenate([cyo[k, 4 * x : 4 * x + 2, :] for x in range(4)], axis=0)
        cyhi[k] = jnp.concatenate([cyo[k, 4 * x + 2 : 4 * x + 4, :] for x in range(4)], axis=0)

    pl.semaphore_wait(barrier, len(nearest))
    greet(rounds.at[0], nearest)

    copies = {}

    def push(name, src, dst, target):
        k = len(copies)
        copies[name] = pltpu.make_async_remote_copy(
            src_ref=src, dst_ref=dst, send_sem=send.at[k], recv_sem=recv.at[k],
            device_id=target, device_id_type=MESH,
        )
        copies[name].start()

    def arrived(*names):
        for name in names:
            copies[name].wait_recv()

    push("zl", opk, zl, device(dz=1))
    push("zr", opk, zr, device(dz=-1))
    blocks = {"v": pl.ds(16, 16), "a": pl.ds(0, 4), "b": pl.ds(4, 4), "c": pl.ds(8, 8), "f": pl.ds(0, 32)}
    up, down, four = pl.ds(6, 2), pl.ds(4, 2), pl.ds(4, 4)

    def push_y(kind):
        rows = blocks[kind]
        near = kind != "f"
        src, dst = (up, pl.ds(2, 2)) if near else (down, pl.ds(0, 2))
        push("yl" + kind, ext.at[four, src, rows], ext.at[four, dst, rows], device(dy=1))
        src, dst = (down, pl.ds(8, 2)) if near else (up, pl.ds(10, 2))
        push("yr" + kind, ext.at[four, src, rows], ext.at[four, dst, rows], device(dy=-1))

    def push_x(kind):
        rows = blocks[kind]
        near = kind != "f"
        src, dst = (up, pl.ds(2, 2)) if near else (down, pl.ds(0, 2))
        push("xl" + kind, ext.at[src, four, rows], ext.at[dst, four, rows], device(dx=1))
        src, dst = (down, pl.ds(8, 2)) if near else (up, pl.ds(10, 2))
        push("xr" + kind, ext.at[src, four, rows], ext.at[dst, four, rows], device(dx=-1))

    for kind in "vabc":
        push_y(kind)
        push_x(kind)
    push("cyl", cyhi, cyl, device(dy=1))
    push("cyr", cylo, cyr, device(dy=-1))
    push("cxl", cxo.at[:, 8:16], cxl, device(dx=1))
    push("cxr", cxo.at[:, 0:8], cxr, device(dx=-1))

    lane16 = lanes(16)
    rim = (lane16 < 2) | (lane16 >= 126)
    rim32 = (lane32 < 2) | (lane32 >= 126)

    def wide(row):
        return jnp.broadcast_to(row, (16, 128))

    def twice(value):
        return jnp.concatenate([value, value], axis=0)

    def rows_of(i):
        return pl.ds(pl.multiple_of(i * 16, 16), 16)

    def density(i, x, y):
        return wide(ext[4 + x, 4 + y, pl.ds(i, 1), :]) * ext[4 + x, 4 + y, 16:32, :]

    def packed(i, k):
        return wide(epk[k, pl.ds(i, 1), :]) * epk[k, 16:32, :]

    def packed_slope(i, at):
        return stencil(*(packed(i, at + k) for k in range(4)))

    def slope_z(n, rims, c):
        sz = stencil(*(rolled(n, -s) for s in SHIFTS))
        return jnp.where(rim, rolled(rims, 124 - 8 * c), sz)

    def keep(factors, at, rows, value):
        factors[at, 0, rows, :], factors[at, 1, rows, :] = split_halves(value)

    def own_columns(i, carry):
        rows = rows_of(i)
        for c in range(16):
            x, y = divmod(c, 4)
            n = density(i, x, y)
            nall[i, x + 2, y + 2] = n
            szb[i, c] = stencil(*(rolled(n, -s) for s in SHIFTS))
            keep(lf, c, rows, n)
        return carry

    lax.fori_loop(0, 16, own_columns, 0)

    arrived("zl", "zr")
    inner32 = lane32 % 8 < 4
    hpk[...] = jnp.where(inner32, zl[0:32, :], zr[0:32, :])
    czh[...] = jnp.where(lanes(8) % 8 < 4, zl[32:40, :], zr[32:40, :])

    def edges(at, opack, hpack):
        high = jnp.where(inner32, opack, hpack)
        low = jnp.where(inner32, hpack, opack)
        for k, s in enumerate(SHIFTS):
            epk[at + k] = jnp.where(inner32, rolled(high, -s), rolled(low, -s))

    edges(0, opk[0:32, :], hpk[...])

    def corners():
        for name, src, dst, target in (
            ("cll", ext.at[up, pl.ds(2, 2)], ext.at[pl.ds(2, 2), pl.ds(2, 2)], 1),
            ("clr", ext.at[up, pl.ds(8, 2)], ext.at[pl.ds(2, 2), pl.ds(8, 2)], 1),
            ("crl", ext.at[down, pl.ds(2, 2)], ext.at[pl.ds(8, 2), pl.ds(2, 2)], -1),
            ("crr", ext.at[down, pl.ds(8, 2)], ext.at[pl.ds(8, 2), pl.ds(8, 2)], -1),
        ):
            push(name, src, dst, device(dx=target))

    def coefficients(c, which):
        return (twice(own[k, c]) for k in which)

    def slopes_xz(i, carry):
        rows = rows_of(i)
        rims = packed_slope(i, 0)
        for y in range(4):
            line = {}
            for x in range(-2, 6):
                if 0 <= x < 4:
                    line[x] = nall[i, x + 2, y + 2]
                else:
                    line[x] = density(i, x, y)
                    nall[i, x + 2, y + 2] = line[x]
            for x in range(4):
                c = 4 * x + y
                sx = stencil(*(line[x + s] for s in SHIFTS))
                sz = jnp.where(rim, rolled(rims, 124 - 8 * c), szb[i, c])
                n = line[x]
                f0, f1, f2, f3, g0, g1, g2 = coefficients(c, range(7))
                aligned = g0 * sx + g2 * sz
                scalar = f1 * n + f2 * aligned
                values = (f0 * n + f1 * aligned, g0 * scalar + f3 * sx, g2 * scalar + f3 * sz)
                local_pot[i, c], fxb[i, x + 2, y], fzb[i, c] = values
                fyb[i, x, y + 2] = g1 * scalar
                for term, value in enumerate(values):
                    keep(rf, 16 * term + c, rows, value)
                for term, value in ((1, sx), (2, sz), (3, g1 * scalar)):
                    keep(lf, 16 * term + c, rows, value)
        return carry

    arrived("xlv", "xrv", "xla", "xra", "xlb", "xrb", "xlc", "xrc")
    lax.fori_loop(0, 16, slopes_xz, 0)
    push("hyl", hpk, hyl, device(dy=1))
    push("hyr", hpk, hyr, device(dy=-1))
    push("hxl", hpk, hxl, device(dx=1))
    push("hxr", hpk, hxr, device(dx=-1))
    pl.semaphore_wait(rounds.at[0], len(nearest))
    greet(rounds.at[1], second_round)
    arrived("ylv", "yrv", "yla", "yra")

    def with_sy(i):
        rows = rows_of(i)
        ends = None
        for x in range(4):
            line = {}
            for y in range(-2, 6):
                if 0 <= y < 4:
                    line[y] = nall[i, x + 2, y + 2]
                else:
                    line[y] = density(i, x, y)
                    nall[i, x + 2, y + 2] = line[y]
            for y in range(4):
                c = 4 * x + y
                sy = stencil(*(line[y + s] for s in SHIFTS))
                keep(ly, c, rows, sy)
                e0, e1, e2, e3 = coefficients(c, range(7, 11))
                fxb[i, x + 2, y] += e0 * sy
                flux = fyb[i, x, y + 2] + e1 * sy
                fyb[i, x, y + 2] = flux
                keep(ry, c, rows, flux)
                flux = fzb[i, c] + e2 * sy
                fzb[i, c] = flux
                part = rolled(flux, 4 + 8 * c)
                ends = part if ends is None else jnp.where(lane16 // 8 == c, part, ends)
                local_pot[i, c] += e3 * sy
        fzp[i] = ends

    def product(a, b):
        return lax.dot_general(a, b, (((1,), (1,)), ((), ())), preferred_element_type=F32)

    def product_of(left, left_at, right, right_at, count):
        a, b, c, d = (
            jnp.concatenate([ref[at + k, half, 0:256, :] for k in range(count)], axis=1)
            for ref, at in ((left, left_at), (right, right_at))
            for half in range(2)
        )
        return product(a, c) + product(a, d) + product(b, c)

    def first_pass(j, carry):
        acc[...] += product_of(lf, 6 * j, rf, 6 * j, 6)
        with_sy(2 * j)
        with_sy(2 * j + 1)
        return carry

    acc[...] = jnp.zeros_like(acc)
    lax.fori_loop(0, 2, first_pass, 0)
    arrived("ylb", "yrb")
    lax.fori_loop(2, 4, first_pass, 0)
    arrived("ylc", "yrc")
    push_y("f")
    push_x("f")
    corners()
    pl.semaphore_wait(rounds.at[1], len(second_round))
    greet(rounds.at[2], third_round)
    lax.fori_loop(4, 8, first_pass, 0)

    arrived("hyl", "hyr", "hxl", "hxr", "cyl", "cyr", "cxl", "cxr")
    sums = acc[...] + product_of(ly, 0, ry, 0, 16) + product_of(lf, 48, ly, 0, 16)

    xpack = pack(lambda c: ext[(8 if c // 4 < 2 else 0) + c // 4, 4 + c % 4])
    edges(4, xpack, jnp.where(lane32 < 64, hxr[...], hxl[...]))
    ypack = pack(lambda c: ext[4 + c // 4, (8 if c % 4 < 2 else 0) + c % 4])
    edges(8, ypack, jnp.where(lane32 % 32 < 16, hyr[...], hyl[...]))
    halo = hpk[...]
    high = jnp.where(inner32, opk[0:32, :], halo)
    low = jnp.where(inner32, halo, opk[0:32, :])
    for k, s in enumerate(SHIFTS):
        epk[21 + k] = jnp.where(inner32, rolled(low, -s), rolled(high, -s))
    epk[12] = halo

    for k, s in enumerate(SHIFTS):
        side_x, side_y = (hxr, hyr) if s > 0 else (hxl, hyl)
        inside_x = lane32 < 128 - 32 * s if s > 0 else lane32 >= -32 * s
        inside_y = lane32 % 32 < 32 - 8 * s if s > 0 else lane32 % 32 >= -8 * s
        epk[13 + k] = jnp.where(inside_x, rolled(halo, -32 * s), rolled(side_x[...], -32 * s))
        over = 32 - 8 * s if s > 0 else -32 - 8 * s
        epk[17 + k] = jnp.where(inside_y, rolled(halo, -8 * s), rolled(side_y[...], over))

    eights = jnp.where(lax.broadcasted_iota(jnp.int32, (32, 128), 0) < 16, 1.0, 8.0)
    halo_columns = [(x, y) for x in (-2, -1, 4, 5) for y in range(4)]
    for m, (x, y) in enumerate(halo_columns):
        c = (x % 4) * 4 + y % 4
        for k, s in enumerate(SHIFTS):
            value = ext[4 + x, 4 + y]
            edge = rolled(epk[4 + k], 124 - 8 * c)
            value = jnp.where(rim32, edge, rolled(value, -s))
            shifted[m, k] = value * eights if k < 2 else value

    for k in range(4):
        for r in range(8):
            for side, ref in enumerate((cxl, cxr, cyl, cyr)):
                halo_coef[k, side, r] = jnp.broadcast_to(ref[k, r : r + 1, :], (8, 128))
    for k in range(ngx):
        cas[k] = sums[nb * k : nb * (k + 1), :] * scale

    pl.semaphore_wait(rounds.at[2], len(third_round))
    first = []
    for k in sorted(range(1, ngx), key=lambda k: -min(k, ngx - k)):
        copy = pltpu.make_async_remote_copy(
            src_ref=cas.at[lax.rem(gx + k, ngx)], dst_ref=ra.at[k],
            send_sem=asend.at[k], recv_sem=arecv.at[k],
            device_id=device(dx=k), device_id_type=MESH,
        )
        copy.start()
        first.append(copy)
    second = []

    def hops(k):
        dy, dz = k // ngz, k % ngz
        return 2 * min(dy, ngy - dy) + min(dz, ngz - dz)

    for k in sorted(range(1, nb), key=lambda k: -hops(k)):
        there = device(dy=k // ngz, dz=k % ngz)
        second.append(
            pltpu.make_async_remote_copy(
                src_ref=dbuf.at[there["gy"] * ngz + there["gz"]], dst_ref=rb.at[k],
                send_sem=bsend.at[k], recv_sem=brecv.at[k],
                device_id=there, device_id_type=MESH,
            )
        )

    def reduce_first():
        for copy in first:
            copy.wait_recv()
        part = cas[gx]
        for k in range(1, ngx):
            part = part + ra[k]
        for r in range(nb):
            dbuf[r] = part[r : r + 1, :]
        for copy in second:
            copy.start()

    arrived("xlf", "xrf", "ylf", "yrf")
    arrived("cll", "clr", "crl", "crr")
    inner16 = lane16 % 8 < 4

    def second_pass(i, carry):
        def at(x, y):
            if (0 <= x < 4 and -2 <= y < 6) or (0 <= y < 4 and -2 <= x < 6):
                return nall[i, x + 2, y + 2]
            return nbuf[x + 4, y + 4]

        zedge = (
            wide(czh[0:1, :]) * packed(i, 12)
            + wide(czh[1:2, :]) * packed_slope(i, 13)
            + wide(czh[2:3, :]) * packed_slope(i, 17)
            + wide(czh[3:4, :]) * packed_slope(i, 21)
        )
        rims = packed_slope(i, 8)
        high = jnp.where(inner16, fzp[i], zedge)
        low = jnp.where(inner16, zedge, fzp[i])
        zends = stencil(*(jnp.where(inner16, rolled(high, -s), rolled(low, -s)) for s in SHIFTS))
        for x in (-4, -3, -2, -1, 0, 1, 2, 3, 4, 5, 6, 7):
            if 0 <= x < 4:
                ys = (-4, -3, 6, 7)
            elif -2 <= x < 6:
                ys = (-2, -1, 4, 5)
            else:
                ys = (0, 1, 2, 3)
            for y in ys:
                nbuf[4 + x, 4 + y] = density(i, x, y)

        def halo_flux(x, y, side, row, sz):
            n = at(x, y)
            sx = stencil(*(at(x + s, y) for s in SHIFTS))
            sy = stencil(*(at(x, y + s) for s in SHIFTS))
            c0, c1, c2, c3 = (twice(halo_coef[k, side, row]) for k in range(4))
            return c0 * n + c1 * sx + c2 * sy + c3 * sz

        for x in (-2, -1, 4, 5):
            for y in range(4):
                m = halo_columns.index((x, y))
                moved = [wide(shifted[m, k, pl.ds(i, 1), :]) * shifted[m, k, 16:32, :] for k in range(4)]
                sz = (moved[0] - moved[1]) - (moved[2] - moved[3])
                side, row = (0, (x + 2) * 4 + y) if x < 0 else (1, (x - 4) * 4 + y)
                fxb[i, x + 2, y] = halo_flux(x, y, side, row, sz)
        for x in range(4):
            for y in (-2, -1, 4, 5):
                sz = slope_z(at(x, y), rims, 4 * x + y % 4)
                side, row = (2, x * 2 + y + 2) if y < 0 else (3, x * 2 + y - 4)
                fyb[i, x, y + 2] = halo_flux(x, y, side, row, sz)

        for c in range(16):
            x, y = divmod(c, 4)
            dx = stencil(*(fxb[i, x + 2 + s, y] for s in SHIFTS))
            dy = stencil(*(fyb[i, x, y + 2 + s] for s in SHIFTS))
            flux = fzb[i, c]
            dz = stencil(*(rolled(flux, -s) for s in SHIFTS))
            dz = jnp.where(rim, rolled(zends, 124 - 8 * c), dz)
            pot[pl.ds(i * 256 + c, 16, stride=16), :] = local_pot[i, c] - (dx + dy + dz)
        return carry

    lax.fori_loop(0, 8, second_pass, 0)
    reduce_first()
    lax.fori_loop(8, 16, second_pass, 0)

    for copy in second:
        copy.wait_recv()
    row = dbuf[gy * ngz + gz]
    for k in range(1, nb):
        row = row + rb[k]
    cas_out[...] = row
    for copy in (*copies.values(), *first, *second):
        copy.wait_send()


def on_device(sizes, scale, occupied, virtual, kernel_fields, density_grad):
    ngx, ngy, ngz = sizes
    nb = ngy * ngz
    vmem = pltpu.VMEM
    dma = pltpu.SemaphoreType.DMA
    scratch = [
        vmem((12, 12, 32, 128), F32), vmem((11, 16, 8, 128), F32),
        vmem((4, 16, 128), F32), vmem((4, 8, 128), F32), vmem((4, 8, 128), F32),
        vmem((4, 16, 128), F32), vmem((4, 8, 128), F32), vmem((4, 8, 128), F32),
        vmem((4, 8, 128), F32), vmem((4, 8, 128), F32),
        vmem((40, 128), F32), vmem((40, 128), F32), vmem((40, 128), F32),
        vmem((32, 128), F32), vmem((32, 128), F32), vmem((32, 128), F32),
        vmem((32, 128), F32), vmem((32, 128), F32), vmem((8, 128), F32),
        vmem((25, 32, 128), F32),
        vmem((16, 8, 8, 16, 128), F32), vmem((12, 12, 16, 128), F32),
        vmem((16, 16, 16, 128), F32), vmem((16, 16, 128), F32),
        vmem((16, 4, 32, 128), F32), vmem((4, 4, 8, 8, 128), F32),
        vmem((16, 8, 4, 16, 128), F32), vmem((16, 4, 8, 16, 128), F32), vmem((16, 16, 16, 128), F32),
        vmem((16, 16, 16, 128), F32),
        vmem((64, 2, 272, 128), BF16), vmem((48, 2, 272, 128), BF16),
        vmem((16, 2, 272, 128), BF16), vmem((16, 2, 272, 128), BF16), vmem((256, 256), F32),
        vmem((ngx, nb, 256), F32), vmem((ngx, nb, 256), F32),
        vmem((nb, 1, 256), F32), vmem((nb, 1, 256), F32),
        dma((36,)), dma((36,)), dma((ngx,)), dma((ngx,)), dma((nb,)), dma((nb,)),
        pltpu.SemaphoreType.REGULAR((3,)),
    ]
    inner = pl.BlockSpec(memory_space=pltpu.VMEM)
    potential, row = pl.pallas_call(
        functools.partial(kernel, sizes, scale),
        out_shape=(
            jax.ShapeDtypeStruct((4096, 128), F32),
            jax.ShapeDtypeStruct((1, 256), F32),
        ),
        in_specs=[inner],
        out_specs=(inner, inner),
        scratch_shapes=scratch,
        compiler_params=pltpu.CompilerParams(
            collective_id=0, has_side_effects=True, vmem_limit_bytes=50 * 1024 * 1024
        ),
    )(jnp.concatenate([occupied, virtual, kernel_fields, density_grad], axis=0).reshape(624, 128))
    return potential.reshape(256, 4, 4, 128), row


def solution(mesh):
    sizes = tuple(mesh.shape[axis] for axis in ("gx", "gy", "gz"))
    scale = 1.0 / (2048 * sizes[0] * sizes[1] * sizes[2])
    placed = P(None, "gx", "gy", "gz")
    return jax.shard_map(
        functools.partial(on_device, sizes, scale),
        mesh=mesh,
        in_specs=(placed,) * 4,
        out_specs=(placed, P(("gx", "gy", "gz"), None)),
        check_vma=False,
    )
```

```python
import functools

import jax
import jax.numpy as jnp
from jax import lax
from jax.experimental import pallas as pl
from jax.experimental.pallas import tpu as pltpu
from jax.sharding import PartitionSpec as P

MESH = pl.DeviceIdType.MESH
F32 = jnp.float32
BF16 = jnp.bfloat16
SHIFTS = (1, -1, 2, -2)


def rolled(value, shift):
    shift %= 128
    return value if shift == 0 else pltpu.roll(value, shift, value.ndim - 1)


def lanes(rows):
    return lax.broadcasted_iota(jnp.int32, (rows, 128), 1)


def stencil(plus1, minus1, plus2, minus2):
    return 8.0 * (plus1 - minus1) - (plus2 - minus2)


def split_halves(value):
    high = value.astype(BF16)
    return high, (value - high.astype(F32)).astype(BF16)


def columns_of(x):
    return range(-2, 6) if 0 <= x < 4 else range(4)


def kernel(
    sizes, scale,
    everything,
    pot, cas_out,
    ext, own, cxo, cxl, cxr, cyo, cyhi, cylo, cyl, cyr,
    opk, zl, zr, hpk, hxl, hxr, hyl, hyr, czh, epk,
    nall, nbuf, szb, fzp, shifted, halo_coef, fxb, fyb, fzb, local_pot, lf, rf, ly, ry, acc,
    cas, ra, dbuf, rb,
    send, recv, asend, arecv, bsend, brecv, rounds,
):
    ngx, ngy, ngz = sizes
    gx, gy, gz = lax.axis_index("gx"), lax.axis_index("gy"), lax.axis_index("gz")
    nb = ngy * ngz

    def device(dx=0, dy=0, dz=0):
        return {
            "gx": lax.rem(gx + dx + ngx, ngx),
            "gy": lax.rem(gy + dy + ngy, ngy),
            "gz": lax.rem(gz + dz + ngz, ngz),
        }

    def greet(semaphore, offsets):
        for dx, dy, dz in offsets:
            pl.semaphore_signal(
                semaphore, inc=1, device_id=device(dx, dy, dz), device_id_type=MESH
            )

    nearest = [(0, 0, 1), (0, 0, -1), (0, 1, 0), (0, -1, 0), (1, 0, 0), (-1, 0, 0)]
    second_round = [(2, 0, 0), (-2, 0, 0), (0, 0, 2), (0, 0, -2)]
    second_round += [(0, dy, dz) for dy in (1, -1) for dz in (1, -1)]
    third_round = [(0, 0, 2), (0, 0, -2)]
    barrier = pltpu.get_barrier_semaphore()
    greet(barrier, nearest)

    for c in range(16):
        x, y = divmod(c, 4)
        ext[4 + x, 4 + y, 0:16, :] = everything[pl.ds(c, 16, stride=16), :]
        ext[4 + x, 4 + y, 16:32, :] = everything[pl.ds(256 + c, 16, stride=16), :]

    f0, f1, f2, f3 = (everything[pl.ds(512 + 16 * k, 16), :] for k in range(4))
    g = [everything[pl.ds(576 + 16 * k, 16), :] * (1.0 / 12.0) for k in range(3)]
    f3s = f3 * (1.0 / 144.0)
    crossed = (g[0] * g[1] * f2, g[1] * g[1] * f2 + f3s, g[2] * g[1] * f2, g[1] * f1)
    for k, value in enumerate((f0, f1, f2, f3s, *g, *crossed)):
        for c in range(16):
            own[k, c] = jnp.broadcast_to(value[c : c + 1, :], (8, 128))

    def combined(k):
        parts = [g[k] * f1]
        for other in range(3):
            beta = g[k] * g[other] * f2
            parts.append(beta + f3s if other == k else beta)
        return parts

    lane32 = lanes(32)

    def pack(at):
        total = None
        for c in range(16):
            part = rolled(at(c), 4 + 8 * c)
            total = part if total is None else jnp.where(lane32 // 8 == c, part, total)
        return total

    opk[0:32, :] = pack(lambda c: ext[4 + c // 4, 4 + c % 4])
    row16 = lax.broadcasted_iota(jnp.int32, (16, 128), 0)
    zrows = []
    for value in combined(2):
        turned = pltpu.roll(value, 4, 1, stride=8, stride_axis=0)
        zrows.append(
            jnp.sum(jnp.where(lanes(16) // 8 == row16, turned, 0.0), axis=0, keepdims=True)
        )
    opk[32:40, :] = jnp.concatenate(zrows + zrows, axis=0)
    for k, value in enumerate(combined(0)):
        cxo[k] = value
    for k, value in enumerate(combined(1)):
        cyo[k] = value
    for k in range(4):
        cylo[k] = jnp.concatenate([cyo[k, 4 * x : 4 * x + 2, :] for x in range(4)], axis=0)
        cyhi[k] = jnp.concatenate([cyo[k, 4 * x + 2 : 4 * x + 4, :] for x in range(4)], axis=0)

    pl.semaphore_wait(barrier, len(nearest))
    greet(rounds.at[0], nearest)

    copies = {}

    def push(name, src, dst, target):
        k = len(copies)
        copies[name] = pltpu.make_async_remote_copy(
            src_ref=src, dst_ref=dst, send_sem=send.at[k], recv_sem=recv.at[k],
            device_id=target, device_id_type=MESH,
        )
        copies[name].start()

    def arrived(*names):
        for name in names:
            copies[name].wait_recv()

    push("zl", opk, zl, device(dz=1))
    push("zr", opk, zr, device(dz=-1))
    blocks = {"v": pl.ds(16, 16), "a": pl.ds(0, 4), "b": pl.ds(4, 4), "c": pl.ds(8, 8), "f": pl.ds(0, 32)}
    up, down, four = pl.ds(6, 2), pl.ds(4, 2), pl.ds(4, 4)

    def push_y(kind):
        rows = blocks[kind]
        near = kind != "f"
        src, dst = (up, pl.ds(2, 2)) if near else (down, pl.ds(0, 2))
        push("yl" + kind, ext.at[four, src, rows], ext.at[four, dst, rows], device(dy=1))
        src, dst = (down, pl.ds(8, 2)) if near else (up, pl.ds(10, 2))
        push("yr" + kind, ext.at[four, src, rows], ext.at[four, dst, rows], device(dy=-1))

    def push_x(kind):
        rows = blocks[kind]
        near = kind != "f"
        src, dst = (up, pl.ds(2, 2)) if near else (down, pl.ds(0, 2))
        push("xl" + kind, ext.at[src, four, rows], ext.at[dst, four, rows], device(dx=1))
        src, dst = (down, pl.ds(8, 2)) if near else (up, pl.ds(10, 2))
        push("xr" + kind, ext.at[src, four, rows], ext.at[dst, four, rows], device(dx=-1))

    for kind in "vabc":
        push_y(kind)
        push_x(kind)
    push("cyl", cyhi, cyl, device(dy=1))
    push("cyr", cylo, cyr, device(dy=-1))
    push("cxl", cxo.at[:, 8:16], cxl, device(dx=1))
    push("cxr", cxo.at[:, 0:8], cxr, device(dx=-1))

    lane16 = lanes(16)
    rim = (lane16 < 2) | (lane16 >= 126)
    rim32 = (lane32 < 2) | (lane32 >= 126)

    def wide(row):
        return jnp.broadcast_to(row, (16, 128))

    def twice(value):
        return jnp.concatenate([value, value], axis=0)

    def rows_of(i):
        return pl.ds(pl.multiple_of(i * 16, 16), 16)

    def density(i, x, y):
        return wide(ext[4 + x, 4 + y, pl.ds(i, 1), :]) * ext[4 + x, 4 + y, 16:32, :]

    def packed(i, k):
        return wide(epk[k, pl.ds(i, 1), :]) * epk[k, 16:32, :]

    def packed_slope(i, at):
        return stencil(*(packed(i, at + k) for k in range(4)))

    def slope_z(n, rims, c):
        sz = stencil(*(rolled(n, -s) for s in SHIFTS))
        return jnp.where(rim, rolled(rims, 124 - 8 * c), sz)

    def keep(factors, at, rows, value):
        factors[at, 0, rows, :], factors[at, 1, rows, :] = split_halves(value)

    def own_columns(i, carry):
        rows = rows_of(i)
        for c in range(16):
            x, y = divmod(c, 4)
            n = density(i, x, y)
            nall[i, x + 2, y + 2] = n
            szb[i, c] = stencil(*(rolled(n, -s) for s in SHIFTS))
            keep(lf, c, rows, n)
        return carry

    lax.fori_loop(0, 16, own_columns, 0)

    arrived("zl", "zr")
    pl.semaphore_wait(rounds.at[0], len(nearest))
    greet(rounds.at[1], second_round)
    inner32 = lane32 % 8 < 4
    hpk[...] = jnp.where(inner32, zl[0:32, :], zr[0:32, :])
    czh[...] = jnp.where(lanes(8) % 8 < 4, zl[32:40, :], zr[32:40, :])

    def edges(at, opack, hpack):
        high = jnp.where(inner32, opack, hpack)
        low = jnp.where(inner32, hpack, opack)
        for k, s in enumerate(SHIFTS):
            epk[at + k] = jnp.where(inner32, rolled(high, -s), rolled(low, -s))

    edges(0, opk[0:32, :], hpk[...])

    def corners(tag, rows):
        for name, src, src_y, dst, dst_y, target in (
            ("cll", up, 2, 2, 2, 1), ("clr", up, 8, 2, 8, 1),
            ("crl", down, 2, 8, 2, -1), ("crr", down, 8, 8, 8, -1),
        ):
            push(
                name + tag, ext.at[src, pl.ds(src_y, 2), rows],
                ext.at[pl.ds(dst, 2), pl.ds(dst_y, 2), rows], device(dx=target),
            )

    def coefficients(c, which):
        return (twice(own[k, c]) for k in which)

    def slopes_xz(i, carry):
        rows = rows_of(i)
        rims = packed_slope(i, 0)
        for y in range(4):
            line = {}
            for x in range(-2, 6):
                if 0 <= x < 4:
                    line[x] = nall[i, x + 2, y + 2]
                else:
                    line[x] = density(i, x, y)
                    nall[i, x + 2, y + 2] = line[x]
            for x in range(4):
                c = 4 * x + y
                sx = stencil(*(line[x + s] for s in SHIFTS))
                sz = jnp.where(rim, rolled(rims, 124 - 8 * c), szb[i, c])
                n = line[x]
                f0, f1, f2, f3, g0, g1, g2 = coefficients(c, range(7))
                aligned = g0 * sx + g2 * sz
                scalar = f1 * n + f2 * aligned
                values = (f0 * n + f1 * aligned, g0 * scalar + f3 * sx, g2 * scalar + f3 * sz)
                local_pot[i, c], fxb[i, x + 2, y], fzb[i, c] = values
                fyb[i, x, y + 2] = g1 * scalar
                for term, value in enumerate(values):
                    keep(rf, 16 * term + c, rows, value)
                for term, value in ((1, sx), (2, sz), (3, g1 * scalar)):
                    keep(lf, 16 * term + c, rows, value)
        return carry

    arrived("xlv", "xrv", "xla", "xra", "xlb", "xrb", "xlc", "xrc")
    lax.fori_loop(0, 16, slopes_xz, 0)
    push_x("f")
    push("hyl", hpk, hyl, device(dy=1))
    push("hyr", hpk, hyr, device(dy=-1))
    push("hxl", hpk, hxl, device(dx=1))
    push("hxr", hpk, hxr, device(dx=-1))
    arrived("ylv", "yrv", "yla", "yra")
    corners("v", pl.ds(16, 16))

    def with_sy(i):
        rows = rows_of(i)
        ends = None
        for x in range(4):
            line = {}
            for y in range(-2, 6):
                if 0 <= y < 4:
                    line[y] = nall[i, x + 2, y + 2]
                else:
                    line[y] = density(i, x, y)
                    nall[i, x + 2, y + 2] = line[y]
            for y in range(4):
                c = 4 * x + y
                sy = stencil(*(line[y + s] for s in SHIFTS))
                keep(ly, c, rows, sy)
                e0, e1, e2, e3 = coefficients(c, range(7, 11))
                fxb[i, x + 2, y] += e0 * sy
                flux = fyb[i, x, y + 2] + e1 * sy
                fyb[i, x, y + 2] = flux
                keep(ry, c, rows, flux)
                flux = fzb[i, c] + e2 * sy
                fzb[i, c] = flux
                part = rolled(flux, 4 + 8 * c)
                ends = part if ends is None else jnp.where(lane16 // 8 == c, part, ends)
                local_pot[i, c] += e3 * sy
        fzp[i] = ends

    def product(a, b):
        return lax.dot_general(a, b, (((1,), (1,)), ((), ())), preferred_element_type=F32)

    def product_of(left, left_at, right, right_at, count):
        a, b, c, d = (
            jnp.concatenate([ref[at + k, half, 0:256, :] for k in range(count)], axis=1)
            for ref, at in ((left, left_at), (right, right_at))
            for half in range(2)
        )
        return product(a, c) + product(a, d) + product(b, c)

    def first_pass(j, carry):
        acc[...] += product_of(lf, 6 * j, rf, 6 * j, 6)
        with_sy(2 * j)
        with_sy(2 * j + 1)
        return carry

    acc[...] = jnp.zeros_like(acc)
    lax.fori_loop(0, 2, first_pass, 0)
    arrived("ylb", "yrb")
    push_y("f")
    lax.fori_loop(2, 4, first_pass, 0)
    arrived("ylc", "yrc")
    corners("o", pl.ds(0, 16))
    lax.fori_loop(4, 8, first_pass, 0)
    pl.semaphore_wait(rounds.at[1], len(second_round))
    greet(rounds.at[2], third_round)

    arrived("hyl", "hyr", "hxl", "hxr", "cyl", "cyr", "cxl", "cxr")
    sums = acc[...] + product_of(ly, 0, ry, 0, 16) + product_of(lf, 48, ly, 0, 16)

    xpack = pack(lambda c: ext[(8 if c // 4 < 2 else 0) + c // 4, 4 + c % 4])
    edges(4, xpack, jnp.where(lane32 < 64, hxr[...], hxl[...]))
    ypack = pack(lambda c: ext[4 + c // 4, (8 if c % 4 < 2 else 0) + c % 4])
    edges(8, ypack, jnp.where(lane32 % 32 < 16, hyr[...], hyl[...]))
    halo = hpk[...]
    high = jnp.where(inner32, opk[0:32, :], halo)
    low = jnp.where(inner32, halo, opk[0:32, :])
    for k, s in enumerate(SHIFTS):
        epk[21 + k] = jnp.where(inner32, rolled(low, -s), rolled(high, -s))
    epk[12] = halo

    for k, s in enumerate(SHIFTS):
        side_x, side_y = (hxr, hyr) if s > 0 else (hxl, hyl)
        inside_x = lane32 < 128 - 32 * s if s > 0 else lane32 >= -32 * s
        inside_y = lane32 % 32 < 32 - 8 * s if s > 0 else lane32 % 32 >= -8 * s
        epk[13 + k] = jnp.where(inside_x, rolled(halo, -32 * s), rolled(side_x[...], -32 * s))
        over = 32 - 8 * s if s > 0 else -32 - 8 * s
        epk[17 + k] = jnp.where(inside_y, rolled(halo, -8 * s), rolled(side_y[...], over))

    eights = jnp.where(lax.broadcasted_iota(jnp.int32, (32, 128), 0) < 16, 1.0, 8.0)
    halo_columns = [(x, y) for x in (-2, -1, 4, 5) for y in range(4)]
    for m, (x, y) in enumerate(halo_columns):
        c = (x % 4) * 4 + y % 4
        for k, s in enumerate(SHIFTS):
            value = ext[4 + x, 4 + y]
            edge = rolled(epk[4 + k], 124 - 8 * c)
            value = jnp.where(rim32, edge, rolled(value, -s))
            shifted[m, k] = value * eights if k < 2 else value

    for k in range(4):
        for r in range(8):
            for side, ref in enumerate((cxl, cxr, cyl, cyr)):
                halo_coef[k, side, r] = jnp.broadcast_to(ref[k, r : r + 1, :], (8, 128))
    for k in range(ngx):
        cas[k] = sums[nb * k : nb * (k + 1), :] * scale

    first = []
    for k in sorted(range(1, ngx), key=lambda k: -min(k, ngx - k)):
        copy = pltpu.make_async_remote_copy(
            src_ref=cas.at[lax.rem(gx + k, ngx)], dst_ref=ra.at[k],
            send_sem=asend.at[k], recv_sem=arecv.at[k],
            device_id=device(dx=k), device_id_type=MESH,
        )
        copy.start()
        first.append(copy)
    second = []

    def hops(k):
        dy, dz = k // ngz, k % ngz
        return 2 * min(dy, ngy - dy) + min(dz, ngz - dz)

    for k in sorted(range(1, nb), key=lambda k: -hops(k)):
        there = device(dy=k // ngz, dz=k % ngz)
        second.append(
            pltpu.make_async_remote_copy(
                src_ref=dbuf.at[there["gy"] * ngz + there["gz"]], dst_ref=rb.at[k],
                send_sem=bsend.at[k], recv_sem=brecv.at[k],
                device_id=there, device_id_type=MESH,
            )
        )

    def reduce_first():
        for copy in first:
            copy.wait_recv()
        part = cas[gx]
        for k in range(1, ngx):
            part = part + ra[k]
        for r in range(nb):
            dbuf[r] = part[r : r + 1, :]
        pl.semaphore_wait(rounds.at[2], len(third_round))
        for copy in second:
            copy.start()

    arrived("xlf", "xrf", "ylf", "yrf")
    arrived("cllv", "clrv", "crlv", "crrv", "cllo", "clro", "crlo", "crro")
    inner16 = lane16 % 8 < 4

    def second_pass(i, carry):
        def at(x, y):
            if (0 <= x < 4 and -2 <= y < 6) or (0 <= y < 4 and -2 <= x < 6):
                return nall[i, x + 2, y + 2]
            return nbuf[x + 4, y + 4]

        zedge = (
            wide(czh[0:1, :]) * packed(i, 12)
            + wide(czh[1:2, :]) * packed_slope(i, 13)
            + wide(czh[2:3, :]) * packed_slope(i, 17)
            + wide(czh[3:4, :]) * packed_slope(i, 21)
        )
        rims = packed_slope(i, 8)
        high = jnp.where(inner16, fzp[i], zedge)
        low = jnp.where(inner16, zedge, fzp[i])
        zends = stencil(*(jnp.where(inner16, rolled(high, -s), rolled(low, -s)) for s in SHIFTS))
        for x in (-4, -3, -2, -1, 0, 1, 2, 3, 4, 5, 6, 7):
            if 0 <= x < 4:
                ys = (-4, -3, 6, 7)
            elif -2 <= x < 6:
                ys = (-2, -1, 4, 5)
            else:
                ys = (0, 1, 2, 3)
            for y in ys:
                nbuf[4 + x, 4 + y] = density(i, x, y)

        def halo_flux(x, y, side, row, sz):
            n = at(x, y)
            sx = stencil(*(at(x + s, y) for s in SHIFTS))
            sy = stencil(*(at(x, y + s) for s in SHIFTS))
            c0, c1, c2, c3 = (twice(halo_coef[k, side, row]) for k in range(4))
            return c0 * n + c1 * sx + c2 * sy + c3 * sz

        for x in (-2, -1, 4, 5):
            for y in range(4):
                m = halo_columns.index((x, y))
                moved = [wide(shifted[m, k, pl.ds(i, 1), :]) * shifted[m, k, 16:32, :] for k in range(4)]
                sz = (moved[0] - moved[1]) - (moved[2] - moved[3])
                side, row = (0, (x + 2) * 4 + y) if x < 0 else (1, (x - 4) * 4 + y)
                fxb[i, x + 2, y] = halo_flux(x, y, side, row, sz)
        for x in range(4):
            for y in (-2, -1, 4, 5):
                sz = slope_z(at(x, y), rims, 4 * x + y % 4)
                side, row = (2, x * 2 + y + 2) if y < 0 else (3, x * 2 + y - 4)
                fyb[i, x, y + 2] = halo_flux(x, y, side, row, sz)

        for c in range(16):
            x, y = divmod(c, 4)
            dx = stencil(*(fxb[i, x + 2 + s, y] for s in SHIFTS))
            dy = stencil(*(fyb[i, x, y + 2 + s] for s in SHIFTS))
            flux = fzb[i, c]
            dz = stencil(*(rolled(flux, -s) for s in SHIFTS))
            dz = jnp.where(rim, rolled(zends, 124 - 8 * c), dz)
            pot[pl.ds(i * 256 + c, 16, stride=16), :] = local_pot[i, c] - (dx + dy + dz)
        return carry

    lax.fori_loop(0, 8, second_pass, 0)
    reduce_first()
    lax.fori_loop(8, 16, second_pass, 0)

    for copy in second:
        copy.wait_recv()
    row = dbuf[gy * ngz + gz]
    for k in range(1, nb):
        row = row + rb[k]
    cas_out[...] = row
    for copy in (*copies.values(), *first, *second):
        copy.wait_send()


def on_device(sizes, scale, occupied, virtual, kernel_fields, density_grad):
    ngx, ngy, ngz = sizes
    nb = ngy * ngz
    vmem = pltpu.VMEM
    dma = pltpu.SemaphoreType.DMA
    scratch = [
        vmem((12, 12, 32, 128), F32), vmem((11, 16, 8, 128), F32),
        vmem((4, 16, 128), F32), vmem((4, 8, 128), F32), vmem((4, 8, 128), F32),
        vmem((4, 16, 128), F32), vmem((4, 8, 128), F32), vmem((4, 8, 128), F32),
        vmem((4, 8, 128), F32), vmem((4, 8, 128), F32),
        vmem((40, 128), F32), vmem((40, 128), F32), vmem((40, 128), F32),
        vmem((32, 128), F32), vmem((32, 128), F32), vmem((32, 128), F32),
        vmem((32, 128), F32), vmem((32, 128), F32), vmem((8, 128), F32),
        vmem((25, 32, 128), F32),
        vmem((16, 8, 8, 16, 128), F32), vmem((12, 12, 16, 128), F32),
        vmem((16, 16, 16, 128), F32), vmem((16, 16, 128), F32),
        vmem((16, 4, 32, 128), F32), vmem((4, 4, 8, 8, 128), F32),
        vmem((16, 8, 4, 16, 128), F32), vmem((16, 4, 8, 16, 128), F32), vmem((16, 16, 16, 128), F32),
        vmem((16, 16, 16, 128), F32),
        vmem((64, 2, 272, 128), BF16), vmem((48, 2, 272, 128), BF16),
        vmem((16, 2, 272, 128), BF16), vmem((16, 2, 272, 128), BF16), vmem((256, 256), F32),
        vmem((ngx, nb, 256), F32), vmem((ngx, nb, 256), F32),
        vmem((nb, 1, 256), F32), vmem((nb, 1, 256), F32),
        dma((40,)), dma((40,)), dma((ngx,)), dma((ngx,)), dma((nb,)), dma((nb,)),
        pltpu.SemaphoreType.REGULAR((3,)),
    ]
    inner = pl.BlockSpec(memory_space=pltpu.VMEM)
    potential, row = pl.pallas_call(
        functools.partial(kernel, sizes, scale),
        out_shape=(
            jax.ShapeDtypeStruct((4096, 128), F32),
            jax.ShapeDtypeStruct((1, 256), F32),
        ),
        in_specs=[inner],
        out_specs=(inner, inner),
        scratch_shapes=scratch,
        compiler_params=pltpu.CompilerParams(
            collective_id=0, has_side_effects=True, vmem_limit_bytes=50 * 1024 * 1024
        ),
    )(jnp.concatenate([occupied, virtual, kernel_fields, density_grad], axis=0).reshape(624, 128))
    return potential.reshape(256, 4, 4, 128), row


def solution(mesh):
    sizes = tuple(mesh.shape[axis] for axis in ("gx", "gy", "gz"))
    scale = 1.0 / (2048 * sizes[0] * sizes[1] * sizes[2])
    placed = P(None, "gx", "gy", "gz")
    return jax.shard_map(
        functools.partial(on_device, sizes, scale),
        mesh=mesh,
        in_specs=(placed,) * 4,
        out_specs=(placed, P(("gx", "gy", "gz"), None)),
        check_vma=False,
    )
```

```python
import functools

import jax
import jax.numpy as jnp
from jax import lax
from jax.experimental import pallas as pl
from jax.experimental.pallas import tpu as pltpu
from jax.sharding import PartitionSpec as P

MESH = pl.DeviceIdType.MESH
F32 = jnp.float32
BF16 = jnp.bfloat16
SHIFTS = (1, -1, 2, -2)


def rolled(value, shift):
    shift %= 128
    return value if shift == 0 else pltpu.roll(value, shift, value.ndim - 1)


def lanes(rows):
    return lax.broadcasted_iota(jnp.int32, (rows, 128), 1)


def stencil(plus1, minus1, plus2, minus2):
    return 8.0 * (plus1 - minus1) - (plus2 - minus2)


def split_halves(value):
    high = value.astype(BF16)
    return high, (value - high.astype(F32)).astype(BF16)


def columns_of(x):
    return range(-2, 6) if 0 <= x < 4 else range(4)


def kernel(
    sizes, scale,
    everything,
    pot, cas_out,
    ext, own, cxo, cxl, cxr, cyo, cyhi, cylo, cyl, cyr,
    opk, zl, zr, hpk, hxl, hxr, hyl, hyr, czh, epk,
    nall, nbuf, szb, fzp, shifted, halo_coef, fxb, fyb, fzb, local_pot, lf, rf, ly, ry, acc,
    cas, ra, dbuf, rb,
    send, recv, asend, arecv, bsend, brecv, rounds,
):
    ngx, ngy, ngz = sizes
    gx, gy, gz = lax.axis_index("gx"), lax.axis_index("gy"), lax.axis_index("gz")
    nb = ngy * ngz

    def device(dx=0, dy=0, dz=0):
        return {
            "gx": lax.rem(gx + dx + ngx, ngx),
            "gy": lax.rem(gy + dy + ngy, ngy),
            "gz": lax.rem(gz + dz + ngz, ngz),
        }

    def greet(semaphore, offsets):
        for dx, dy, dz in offsets:
            pl.semaphore_signal(
                semaphore, inc=1, device_id=device(dx, dy, dz), device_id_type=MESH
            )

    nearest = [(0, 0, 1), (0, 0, -1), (0, 1, 0), (0, -1, 0), (1, 0, 0), (-1, 0, 0)]
    second_round = [(2, 0, 0), (-2, 0, 0), (0, 0, 2), (0, 0, -2)]
    second_round += [(0, dy, dz) for dy in (1, -1) for dz in (1, -1)]
    third_round = [(0, 0, 2), (0, 0, -2)]
    barrier = pltpu.get_barrier_semaphore()
    greet(barrier, nearest)

    for c in range(16):
        x, y = divmod(c, 4)
        ext[4 + x, 4 + y, 0:16, :] = everything[pl.ds(c, 16, stride=16), :]
        ext[4 + x, 4 + y, 16:32, :] = everything[pl.ds(256 + c, 16, stride=16), :]

    f0, f1, f2, f3 = (everything[pl.ds(512 + 16 * k, 16), :] for k in range(4))
    g = [everything[pl.ds(576 + 16 * k, 16), :] * (1.0 / 12.0) for k in range(3)]
    f3s = f3 * (1.0 / 144.0)
    crossed = (g[0] * g[1] * f2, g[1] * g[1] * f2 + f3s, g[2] * g[1] * f2, g[1] * f1)
    for k, value in enumerate((f0, f1, f2, f3s, *g, *crossed)):
        for c in range(16):
            own[k, c] = jnp.broadcast_to(value[c : c + 1, :], (8, 128))

    def combined(k):
        parts = [g[k] * f1]
        for other in range(3):
            beta = g[k] * g[other] * f2
            parts.append(beta + f3s if other == k else beta)
        return parts

    lane32 = lanes(32)

    def pack(at):
        total = None
        for c in range(16):
            part = rolled(at(c), 4 + 8 * c)
            total = part if total is None else jnp.where(lane32 // 8 == c, part, total)
        return total

    opk[0:32, :] = pack(lambda c: ext[4 + c // 4, 4 + c % 4])
    row16 = lax.broadcasted_iota(jnp.int32, (16, 128), 0)
    zrows = []
    for value in combined(2):
        turned = pltpu.roll(value, 4, 1, stride=8, stride_axis=0)
        zrows.append(
            jnp.sum(jnp.where(lanes(16) // 8 == row16, turned, 0.0), axis=0, keepdims=True)
        )
    opk[32:40, :] = jnp.concatenate(zrows + zrows, axis=0)
    for k, value in enumerate(combined(0)):
        cxo[k] = value
    for k, value in enumerate(combined(1)):
        cyo[k] = value
    for k in range(4):
        cylo[k] = jnp.concatenate([cyo[k, 4 * x : 4 * x + 2, :] for x in range(4)], axis=0)
        cyhi[k] = jnp.concatenate([cyo[k, 4 * x + 2 : 4 * x + 4, :] for x in range(4)], axis=0)

    pl.semaphore_wait(barrier, len(nearest))
    greet(rounds.at[0], nearest)

    copies = {}

    def push(name, src, dst, target):
        k = len(copies)
        copies[name] = pltpu.make_async_remote_copy(
            src_ref=src, dst_ref=dst, send_sem=send.at[k], recv_sem=recv.at[k],
            device_id=target, device_id_type=MESH,
        )
        copies[name].start()

    def arrived(*names):
        for name in names:
            copies[name].wait_recv()

    push("zl", opk, zl, device(dz=1))
    push("zr", opk, zr, device(dz=-1))
    blocks = {"v": pl.ds(16, 16), "a": pl.ds(0, 4), "b": pl.ds(4, 4), "c": pl.ds(8, 8), "f": pl.ds(0, 32), "n": pl.ds(0, 32)}
    up, down, four = pl.ds(6, 2), pl.ds(4, 2), pl.ds(4, 4)

    def push_y(kind):
        rows = blocks[kind]
        near = kind != "f"
        src, dst = (up, pl.ds(2, 2)) if near else (down, pl.ds(0, 2))
        push("yl" + kind, ext.at[four, src, rows], ext.at[four, dst, rows], device(dy=1))
        src, dst = (down, pl.ds(8, 2)) if near else (up, pl.ds(10, 2))
        push("yr" + kind, ext.at[four, src, rows], ext.at[four, dst, rows], device(dy=-1))

    def push_x(kind):
        rows = blocks[kind]
        near = kind != "f"
        src, dst = (up, pl.ds(2, 2)) if near else (down, pl.ds(0, 2))
        push("xl" + kind, ext.at[src, four, rows], ext.at[dst, four, rows], device(dx=1))
        src, dst = (down, pl.ds(8, 2)) if near else (up, pl.ds(10, 2))
        push("xr" + kind, ext.at[src, four, rows], ext.at[dst, four, rows], device(dx=-1))

    push_x("n")
    for kind in "vabc":
        push_y(kind)
    push("cyl", cyhi, cyl, device(dy=1))
    push("cyr", cylo, cyr, device(dy=-1))
    push("cxl", cxo.at[:, 8:16], cxl, device(dx=1))
    push("cxr", cxo.at[:, 0:8], cxr, device(dx=-1))

    lane16 = lanes(16)
    rim = (lane16 < 2) | (lane16 >= 126)
    rim32 = (lane32 < 2) | (lane32 >= 126)

    def wide(row):
        return jnp.broadcast_to(row, (16, 128))

    def twice(value):
        return jnp.concatenate([value, value], axis=0)

    def rows_of(i):
        return pl.ds(pl.multiple_of(i * 16, 16), 16)

    def density(i, x, y):
        return wide(ext[4 + x, 4 + y, pl.ds(i, 1), :]) * ext[4 + x, 4 + y, 16:32, :]

    def packed(i, k):
        return wide(epk[k, pl.ds(i, 1), :]) * epk[k, 16:32, :]

    def packed_slope(i, at):
        return stencil(*(packed(i, at + k) for k in range(4)))

    def slope_z(n, rims, c):
        sz = stencil(*(rolled(n, -s) for s in SHIFTS))
        return jnp.where(rim, rolled(rims, 124 - 8 * c), sz)

    def keep(factors, at, rows, value):
        factors[at, 0, rows, :], factors[at, 1, rows, :] = split_halves(value)

    def own_columns(i, carry):
        rows = rows_of(i)
        for c in range(16):
            x, y = divmod(c, 4)
            n = density(i, x, y)
            nall[i, x + 2, y + 2] = n
            szb[i, c] = stencil(*(rolled(n, -s) for s in SHIFTS))
            keep(lf, c, rows, n)
        return carry

    lax.fori_loop(0, 16, own_columns, 0)

    arrived("zl", "zr")
    pl.semaphore_wait(rounds.at[0], len(nearest))
    greet(rounds.at[1], second_round)
    inner32 = lane32 % 8 < 4
    hpk[...] = jnp.where(inner32, zl[0:32, :], zr[0:32, :])
    czh[...] = jnp.where(lanes(8) % 8 < 4, zl[32:40, :], zr[32:40, :])

    def edges(at, opack, hpack):
        high = jnp.where(inner32, opack, hpack)
        low = jnp.where(inner32, hpack, opack)
        for k, s in enumerate(SHIFTS):
            epk[at + k] = jnp.where(inner32, rolled(high, -s), rolled(low, -s))

    edges(0, opk[0:32, :], hpk[...])

    def corners(tag, rows):
        for name, src, src_y, dst, dst_y, target in (
            ("cll", up, 2, 2, 2, 1), ("clr", up, 8, 2, 8, 1),
            ("crl", down, 2, 8, 2, -1), ("crr", down, 8, 8, 8, -1),
        ):
            push(
                name + tag, ext.at[src, pl.ds(src_y, 2), rows],
                ext.at[pl.ds(dst, 2), pl.ds(dst_y, 2), rows], device(dx=target),
            )

    def coefficients(c, which):
        return (twice(own[k, c]) for k in which)

    def slopes_xz(i, carry):
        rows = rows_of(i)
        rims = packed_slope(i, 0)
        for y in range(4):
            line = {}
            for x in range(-2, 6):
                if 0 <= x < 4:
                    line[x] = nall[i, x + 2, y + 2]
                else:
                    line[x] = density(i, x, y)
                    nall[i, x + 2, y + 2] = line[x]
            for x in range(4):
                c = 4 * x + y
                sx = stencil(*(line[x + s] for s in SHIFTS))
                sz = jnp.where(rim, rolled(rims, 124 - 8 * c), szb[i, c])
                n = line[x]
                f0, f1, f2, f3, g0, g1, g2 = coefficients(c, range(7))
                aligned = g0 * sx + g2 * sz
                scalar = f1 * n + f2 * aligned
                values = (f0 * n + f1 * aligned, g0 * scalar + f3 * sx, g2 * scalar + f3 * sz)
                local_pot[i, c], fxb[i, x + 2, y], fzb[i, c] = values
                fyb[i, x, y + 2] = g1 * scalar
                for term, value in enumerate(values):
                    keep(rf, 16 * term + c, rows, value)
                for term, value in ((1, sx), (2, sz), (3, g1 * scalar)):
                    keep(lf, 16 * term + c, rows, value)
        return carry

    arrived("xln", "xrn")
    lax.fori_loop(0, 16, slopes_xz, 0)
    push_x("f")
    push("hyl", hpk, hyl, device(dy=1))
    push("hyr", hpk, hyr, device(dy=-1))
    push("hxl", hpk, hxl, device(dx=1))
    push("hxr", hpk, hxr, device(dx=-1))
    arrived("ylv", "yrv", "yla", "yra")
    corners("v", pl.ds(16, 16))

    def with_sy(i):
        rows = rows_of(i)
        ends = None
        for x in range(4):
            line = {}
            for y in range(-2, 6):
                if 0 <= y < 4:
                    line[y] = nall[i, x + 2, y + 2]
                else:
                    line[y] = density(i, x, y)
                    nall[i, x + 2, y + 2] = line[y]
            for y in range(4):
                c = 4 * x + y
                sy = stencil(*(line[y + s] for s in SHIFTS))
                keep(ly, c, rows, sy)
                e0, e1, e2, e3 = coefficients(c, range(7, 11))
                fxb[i, x + 2, y] += e0 * sy
                flux = fyb[i, x, y + 2] + e1 * sy
                fyb[i, x, y + 2] = flux
                keep(ry, c, rows, flux)
                flux = fzb[i, c] + e2 * sy
                fzb[i, c] = flux
                part = rolled(flux, 4 + 8 * c)
                ends = part if ends is None else jnp.where(lane16 // 8 == c, part, ends)
                local_pot[i, c] += e3 * sy
        fzp[i] = ends

    def product(a, b):
        return lax.dot_general(a, b, (((1,), (1,)), ((), ())), preferred_element_type=F32)

    def product_of(left, left_at, right, right_at, count):
        a, b, c, d = (
            jnp.concatenate([ref[at + k, half, 0:256, :] for k in range(count)], axis=1)
            for ref, at in ((left, left_at), (right, right_at))
            for half in range(2)
        )
        return product(a, c) + product(a, d) + product(b, c)

    def first_pass(j, carry):
        acc[...] += product_of(lf, 6 * j, rf, 6 * j, 6)
        with_sy(2 * j)
        with_sy(2 * j + 1)
        return carry

    acc[...] = jnp.zeros_like(acc)
    lax.fori_loop(0, 2, first_pass, 0)
    arrived("ylb", "yrb")
    push_y("f")
    lax.fori_loop(2, 4, first_pass, 0)
    arrived("ylc", "yrc")
    corners("o", pl.ds(0, 16))
    lax.fori_loop(4, 8, first_pass, 0)
    pl.semaphore_wait(rounds.at[1], len(second_round))
    greet(rounds.at[2], third_round)

    arrived("hyl", "hyr", "hxl", "hxr", "cyl", "cyr", "cxl", "cxr")
    sums = acc[...] + product_of(ly, 0, ry, 0, 16) + product_of(lf, 48, ly, 0, 16)

    xpack = pack(lambda c: ext[(8 if c // 4 < 2 else 0) + c // 4, 4 + c % 4])
    edges(4, xpack, jnp.where(lane32 < 64, hxr[...], hxl[...]))
    ypack = pack(lambda c: ext[4 + c // 4, (8 if c % 4 < 2 else 0) + c % 4])
    edges(8, ypack, jnp.where(lane32 % 32 < 16, hyr[...], hyl[...]))
    halo = hpk[...]
    high = jnp.where(inner32, opk[0:32, :], halo)
    low = jnp.where(inner32, halo, opk[0:32, :])
    for k, s in enumerate(SHIFTS):
        epk[21 + k] = jnp.where(inner32, rolled(low, -s), rolled(high, -s))
    epk[12] = halo

    for k, s in enumerate(SHIFTS):
        side_x, side_y = (hxr, hyr) if s > 0 else (hxl, hyl)
        inside_x = lane32 < 128 - 32 * s if s > 0 else lane32 >= -32 * s
        inside_y = lane32 % 32 < 32 - 8 * s if s > 0 else lane32 % 32 >= -8 * s
        epk[13 + k] = jnp.where(inside_x, rolled(halo, -32 * s), rolled(side_x[...], -32 * s))
        over = 32 - 8 * s if s > 0 else -32 - 8 * s
        epk[17 + k] = jnp.where(inside_y, rolled(halo, -8 * s), rolled(side_y[...], over))

    eights = jnp.where(lax.broadcasted_iota(jnp.int32, (32, 128), 0) < 16, 1.0, 8.0)
    halo_columns = [(x, y) for x in (-2, -1, 4, 5) for y in range(4)]
    for m, (x, y) in enumerate(halo_columns):
        c = (x % 4) * 4 + y % 4
        for k, s in enumerate(SHIFTS):
            value = ext[4 + x, 4 + y]
            edge = rolled(epk[4 + k], 124 - 8 * c)
            value = jnp.where(rim32, edge, rolled(value, -s))
            shifted[m, k] = value * eights if k < 2 else value

    for k in range(4):
        for r in range(8):
            for side, ref in enumerate((cxl, cxr, cyl, cyr)):
                halo_coef[k, side, r] = jnp.broadcast_to(ref[k, r : r + 1, :], (8, 128))
    for k in range(ngx):
        cas[k] = sums[nb * k : nb * (k + 1), :] * scale

    first = []
    for k in sorted(range(1, ngx), key=lambda k: -min(k, ngx - k)):
        copy = pltpu.make_async_remote_copy(
            src_ref=cas.at[lax.rem(gx + k, ngx)], dst_ref=ra.at[k],
            send_sem=asend.at[k], recv_sem=arecv.at[k],
            device_id=device(dx=k), device_id_type=MESH,
        )
        copy.start()
        first.append(copy)
    second = []

    def hops(k):
        dy, dz = k // ngz, k % ngz
        return 2 * min(dy, ngy - dy) + min(dz, ngz - dz)

    for k in sorted(range(1, nb), key=lambda k: -hops(k)):
        there = device(dy=k // ngz, dz=k % ngz)
        second.append(
            pltpu.make_async_remote_copy(
                src_ref=dbuf.at[there["gy"] * ngz + there["gz"]], dst_ref=rb.at[k],
                send_sem=bsend.at[k], recv_sem=brecv.at[k],
                device_id=there, device_id_type=MESH,
            )
        )

    def reduce_first():
        for copy in first:
            copy.wait_recv()
        part = cas[gx]
        for k in range(1, ngx):
            part = part + ra[k]
        for r in range(nb):
            dbuf[r] = part[r : r + 1, :]
        pl.semaphore_wait(rounds.at[2], len(third_round))
        for copy in second:
            copy.start()

    arrived("xlf", "xrf", "ylf", "yrf")
    arrived("cllv", "clrv", "crlv", "crrv", "cllo", "clro", "crlo", "crro")
    inner16 = lane16 % 8 < 4

    def second_pass(i, carry):
        def at(x, y):
            if (0 <= x < 4 and -2 <= y < 6) or (0 <= y < 4 and -2 <= x < 6):
                return nall[i, x + 2, y + 2]
            return nbuf[x + 4, y + 4]

        zedge = (
            wide(czh[0:1, :]) * packed(i, 12)
            + wide(czh[1:2, :]) * packed_slope(i, 13)
            + wide(czh[2:3, :]) * packed_slope(i, 17)
            + wide(czh[3:4, :]) * packed_slope(i, 21)
        )
        rims = packed_slope(i, 8)
        high = jnp.where(inner16, fzp[i], zedge)
        low = jnp.where(inner16, zedge, fzp[i])
        zends = stencil(*(jnp.where(inner16, rolled(high, -s), rolled(low, -s)) for s in SHIFTS))
        for x in (-4, -3, -2, -1, 0, 1, 2, 3, 4, 5, 6, 7):
            if 0 <= x < 4:
                ys = (-4, -3, 6, 7)
            elif -2 <= x < 6:
                ys = (-2, -1, 4, 5)
            else:
                ys = (0, 1, 2, 3)
            for y in ys:
                nbuf[4 + x, 4 + y] = density(i, x, y)

        def halo_flux(x, y, side, row, sz):
            n = at(x, y)
            sx = stencil(*(at(x + s, y) for s in SHIFTS))
            sy = stencil(*(at(x, y + s) for s in SHIFTS))
            c0, c1, c2, c3 = (twice(halo_coef[k, side, row]) for k in range(4))
            return c0 * n + c1 * sx + c2 * sy + c3 * sz

        for x in (-2, -1, 4, 5):
            for y in range(4):
                m = halo_columns.index((x, y))
                moved = [wide(shifted[m, k, pl.ds(i, 1), :]) * shifted[m, k, 16:32, :] for k in range(4)]
                sz = (moved[0] - moved[1]) - (moved[2] - moved[3])
                side, row = (0, (x + 2) * 4 + y) if x < 0 else (1, (x - 4) * 4 + y)
                fxb[i, x + 2, y] = halo_flux(x, y, side, row, sz)
        for x in range(4):
            for y in (-2, -1, 4, 5):
                sz = slope_z(at(x, y), rims, 4 * x + y % 4)
                side, row = (2, x * 2 + y + 2) if y < 0 else (3, x * 2 + y - 4)
                fyb[i, x, y + 2] = halo_flux(x, y, side, row, sz)

        for c in range(16):
            x, y = divmod(c, 4)
            dx = stencil(*(fxb[i, x + 2 + s, y] for s in SHIFTS))
            dy = stencil(*(fyb[i, x, y + 2 + s] for s in SHIFTS))
            flux = fzb[i, c]
            dz = stencil(*(rolled(flux, -s) for s in SHIFTS))
            dz = jnp.where(rim, rolled(zends, 124 - 8 * c), dz)
            pot[pl.ds(i * 256 + c, 16, stride=16), :] = local_pot[i, c] - (dx + dy + dz)
        return carry

    lax.fori_loop(0, 8, second_pass, 0)
    reduce_first()
    lax.fori_loop(8, 16, second_pass, 0)

    for copy in second:
        copy.wait_recv()
    row = dbuf[gy * ngz + gz]
    for k in range(1, nb):
        row = row + rb[k]
    cas_out[...] = row
    for copy in (*copies.values(), *first, *second):
        copy.wait_send()


def on_device(sizes, scale, occupied, virtual, kernel_fields, density_grad):
    ngx, ngy, ngz = sizes
    nb = ngy * ngz
    vmem = pltpu.VMEM
    dma = pltpu.SemaphoreType.DMA
    scratch = [
        vmem((12, 12, 32, 128), F32), vmem((11, 16, 8, 128), F32),
        vmem((4, 16, 128), F32), vmem((4, 8, 128), F32), vmem((4, 8, 128), F32),
        vmem((4, 16, 128), F32), vmem((4, 8, 128), F32), vmem((4, 8, 128), F32),
        vmem((4, 8, 128), F32), vmem((4, 8, 128), F32),
        vmem((40, 128), F32), vmem((40, 128), F32), vmem((40, 128), F32),
        vmem((32, 128), F32), vmem((32, 128), F32), vmem((32, 128), F32),
        vmem((32, 128), F32), vmem((32, 128), F32), vmem((8, 128), F32),
        vmem((25, 32, 128), F32),
        vmem((16, 8, 8, 16, 128), F32), vmem((12, 12, 16, 128), F32),
        vmem((16, 16, 16, 128), F32), vmem((16, 16, 128), F32),
        vmem((16, 4, 32, 128), F32), vmem((4, 4, 8, 8, 128), F32),
        vmem((16, 8, 4, 16, 128), F32), vmem((16, 4, 8, 16, 128), F32), vmem((16, 16, 16, 128), F32),
        vmem((16, 16, 16, 128), F32),
        vmem((64, 2, 272, 128), BF16), vmem((48, 2, 272, 128), BF16),
        vmem((16, 2, 272, 128), BF16), vmem((16, 2, 272, 128), BF16), vmem((256, 256), F32),
        vmem((ngx, nb, 256), F32), vmem((ngx, nb, 256), F32),
        vmem((nb, 1, 256), F32), vmem((nb, 1, 256), F32),
        dma((40,)), dma((40,)), dma((ngx,)), dma((ngx,)), dma((nb,)), dma((nb,)),
        pltpu.SemaphoreType.REGULAR((3,)),
    ]
    inner = pl.BlockSpec(memory_space=pltpu.VMEM)
    potential, row = pl.pallas_call(
        functools.partial(kernel, sizes, scale),
        out_shape=(
            jax.ShapeDtypeStruct((4096, 128), F32),
            jax.ShapeDtypeStruct((1, 256), F32),
        ),
        in_specs=[inner],
        out_specs=(inner, inner),
        scratch_shapes=scratch,
        compiler_params=pltpu.CompilerParams(
            collective_id=0, has_side_effects=True, vmem_limit_bytes=50 * 1024 * 1024
        ),
    )(jnp.concatenate([occupied, virtual, kernel_fields, density_grad], axis=0).reshape(624, 128))
    return potential.reshape(256, 4, 4, 128), row


def solution(mesh):
    sizes = tuple(mesh.shape[axis] for axis in ("gx", "gy", "gz"))
    scale = 1.0 / (2048 * sizes[0] * sizes[1] * sizes[2])
    placed = P(None, "gx", "gy", "gz")
    return jax.shard_map(
        functools.partial(on_device, sizes, scale),
        mesh=mesh,
        in_specs=(placed,) * 4,
        out_specs=(placed, P(("gx", "gy", "gz"), None)),
        check_vma=False,
    )
```
